32 devices in a mesh: dp: 8 (over y, x, core), seq: 4 (over z).
Axes of the slice: x: 2, y: 2, z: 4, core: 2. Of those that a mesh axis runs over, the one named last changes fastest.
Arguments:
- atom_single: bfloat16 [16, 4096, 128], P('dp', 'seq'), may hold values from -6 to 6
- atom_cond: bfloat16 [16, 4096, 128], P('dp', 'seq'), may hold values from -6 to 6
- token_single: bfloat16 [16, 512, 768], P('dp', 'seq'), may hold values from -6 to 6
- token_cond: bfloat16 [16, 512, 384], P('dp', 'seq'), may hold values from -6 to 6
- atom_pair: bfloat16 [128, 32, 2048], P('seq'), may hold values from -6 to 6
- token_pair: bfloat16 [512, 512, 128], P('seq', 'dp'), may hold values from -6 to 6
- atom_token: int32 [4096], P('seq'), may hold values from 0 to 511, as said below
- window_shift: int32 [128], P('seq'), may hold values from -16 to 16
- noise_bin: int32 [16], P('dp'), may hold values from 0 to 63
- out_cotangent: bfloat16 [16, 512, 768], P('dp', 'seq'), may hold values from -6 to 6
- atom_cond_weight: bfloat16 [128, 768], replicated, may hold values from -0.5 to 0.5
- atom_scale_bias: bfloat16 [256], replicated, may hold values from -4 to 4
- atom_zero_bias: bfloat16 [256], replicated, may hold values from -4 to 4
- atom_projection: bfloat16 [128, 512], replicated, may hold values from -0.5 to 0.5
- atom_output: bfloat16 [128, 128], replicated, may hold values from -1.5 to 1.5
- atom_pair_weight: bfloat16 [16, 4], replicated, may hold values from -1.5 to 1.5
- atom_up_weight: bfloat16 [128, 512], replicated, may hold values from -0.5 to 0.5
- atom_down_weight: bfloat16 [256, 128], replicated, may hold values from -0.375 to 0.375
- pool_weight: bfloat16 [128, 768], replicated, may hold values from -0.5 to 0.5
- cond_weight: bfloat16 [384, 4608], P('seq'), may hold values from -0.3125 to 0.3125
- scale_bias: bfloat16 [1536], replicated, may hold values from -4 to 4
- zero_bias: bfloat16 [1536], replicated, may hold values from -4 to 4
- token_projection: bfloat16 [768, 3072], P('seq'), may hold values from -0.21875 to 0.21875
- token_output: bfloat16 [768, 768], P('seq'), may hold values from -0.875 to 0.875
- token_pair_weight: bfloat16 [128, 16], replicated, may hold values from -0.5 to 0.5
- token_up_weight: bfloat16 [768, 3072], P('seq'), may hold values from -0.21875 to 0.21875
- token_down_weight: bfloat16 [1536, 768], P('seq'), may hold values from -0.15625 to 0.15625
Outputs:
- block_out: bfloat16 [16, 512, 768], P('dp', 'seq')
- grad_atom_single: float32 [16, 4096, 128], P('dp', 'seq')
- grad_atom_cond: float32 [16, 4096, 128], P('dp', 'seq')
- grad_token_single: float32 [16, 512, 768], P('dp', 'seq')
- grad_token_cond: float32 [16, 512, 384], P('dp', 'seq')
- grad_atom_pair: float32 [128, 32, 2048], P('seq')
- grad_token_pair: float32 [512, 512, 128], P('seq', 'dp')
- grad_atom_cond_weight: float32 [128, 768], replicated
- grad_atom_scale_bias: float32 [256], replicated
- grad_atom_zero_bias: float32 [256], replicated
- grad_atom_projection: float32 [128, 512], replicated
- grad_atom_output: float32 [128, 128], replicated
- grad_atom_pair_weight: float32 [16, 4], replicated
- grad_atom_up_weight: float32 [128, 512], replicated
- grad_atom_down_weight: float32 [256, 128], replicated
- grad_pool_weight: float32 [128, 768], replicated
- grad_cond_weight: float32 [384, 4608], replicated
- grad_scale_bias: float32 [1536], replicated
- grad_zero_bias: float32 [1536], replicated
- grad_token_projection: float32 [768, 3072], replicated
- grad_token_output: float32 [768, 768], replicated
- grad_token_pair_weight: float32 [128, 16], replicated
- grad_token_up_weight: float32 [768, 3072], replicated
- grad_token_down_weight: float32 [1536, 768], replicated
The draws below stay inside these ranges and needn't reach their ends.
Inputs may be any that keep to these rules, and one draw needn't show every extreme that they name: `atom_token`: Non-decreasing; for every k below the number of seq groups, atoms k * 4096 // 4 to (k + 1) * 4096 // 4 - 1 name only tokens k * 512 // 4 to (k + 1) * 512 // 4 - 1, and every token is named by at least one atom.
All inputs are finite; a program needn't handle non-finite values.
Results may differ from the reference program's by a relative error of at most 0.035.
Values may be sent and summed in bfloat16 or wider, within the bound.
A program may use at most 256 MiB of HBM per device.

```python
import math
import jax
import jax.numpy as jnp
from jax import lax

D = 768
H = 16
DH = 48
FF = 1536
CS = 384
CZ = 128
DA = 128
HA = 4
DHA = 32
FFA = 256
CP = 16
WQ = 32
WK = 128
NT = 512
NBIN = 64
SAMPLES = 16
NA = 4096
NWIN = 128
N_SEQ = 4


def draw_atom_token(key, part):
    atoms_block = NA // N_SEQ
    tokens_block = NT // N_SEQ
    extra = jax.random.randint(key, (N_SEQ, atoms_block - tokens_block), 0, tokens_block)
    base = jnp.broadcast_to(jnp.arange(tokens_block, dtype=jnp.int32)[None, :], (N_SEQ, tokens_block))
    local_tokens = jnp.sort(jnp.concatenate([base, extra.astype(jnp.int32)], axis=1), axis=1)
    offsets = jnp.arange(N_SEQ, dtype=jnp.int32)[:, None] * tokens_block
    return (local_tokens + offsets).reshape(NA).astype(jnp.int32)


def draw_window_shift(key, part):
    shifts = jax.random.randint(key, (NWIN,), -(WQ // 2), WQ // 2 + 1)
    return shifts.at[1].set(WQ // 2).at[2].set(-(WQ // 2)).astype(jnp.int32)


def draw_noise_bin(key, part):
    bins = jax.random.randint(key, (SAMPLES,), 0, NBIN)
    return bins.at[0].set(0).at[1].set(NBIN - 1).astype(jnp.int32)


def shard_levels(rng, extent, split, low, top_value):
    gain = 1.0
    for position, shards_of in split:
        steps = jax.random.uniform(jax.random.fold_in(jax.random.fold_in(rng, 6), position), (shards_of,), jnp.float32, low / len(split), top_value / len(split))
        gain = gain * jnp.repeat(jnp.exp(steps), extent[position] // shards_of).reshape((-1,) + (1,) * (len(extent) - 1 - position))
    return gain


def bell_draw(rng, dims, scale, bound, shards=(), held_as=jnp.bfloat16):
    values = jax.random.normal(rng, dims, jnp.float32) * scale
    if len(shards) > 0:
        values = shard_levels(rng, dims, shards, -0.22, 0.18) * values
    return jnp.clip(values, min=-bound, max=bound).astype(held_as)


def setup_inputs(seed: int = 0) -> dict:
    splits = jax.random.split(jax.random.key(seed), 28)
    return {
        "atom_single": bell_draw(splits[0], (SAMPLES, NA, DA), 1.0, 6.0, ((0, 8), (1, 4))),
        "atom_cond": bell_draw(splits[1], (SAMPLES, NA, DA), 1.0, 6.0, ((0, 8), (1, 4))),
        "token_single": bell_draw(splits[2], (SAMPLES, NT, D), 1.0, 6.0, ((0, 8), (1, 4))),
        "token_cond": bell_draw(splits[3], (SAMPLES, NT, CS), 1.0, 6.0, ((0, 8), (1, 4))),
        "atom_pair": bell_draw(splits[4], (NWIN, WQ, WK * CP), 1.0, 6.0, ((0, 4),)),
        "token_pair": bell_draw(splits[5], (NT, NT, CZ), 1.0, 6.0, ((0, 4), (1, 8))),
        "atom_token": draw_atom_token(jax.random.fold_in(splits[27], 71), 0),
        "window_shift": draw_window_shift(jax.random.fold_in(splits[27], 71), 0),
        "noise_bin": draw_noise_bin(jax.random.fold_in(splits[27], 71), 0),
        "out_cotangent": bell_draw(splits[9], (SAMPLES, NT, D), 1.0, 6.0, ((0, 8), (1, 4))),
        "atom_cond_weight": bell_draw(splits[10], (DA, 6 * DA), DA ** -0.5, 0.5),
        "atom_scale_bias": bell_draw(splits[11], (2 * DA,), 1.0, 4.0),
        "atom_zero_bias": bell_draw(splits[12], (2 * DA,), 1.0, 4.0),
        "atom_projection": bell_draw(splits[13], (DA, 4 * DA), DA ** -0.5, 0.5),
        "atom_output": bell_draw(splits[14], (DA, DA), (DA // 8) ** -0.5, 1.5),
        "atom_pair_weight": bell_draw(splits[15], (CP, HA), CP ** -0.5, 1.5),
        "atom_up_weight": bell_draw(splits[16], (DA, 2 * FFA), DA ** -0.5, 0.5),
        "atom_down_weight": bell_draw(splits[17], (FFA, DA), FFA ** -0.5, 0.375),
        "pool_weight": bell_draw(splits[18], (DA, D), DA ** -0.5, 0.5),
        "cond_weight": bell_draw(splits[19], (CS, 6 * D), CS ** -0.5, 0.3125, ((0, 4),)),
        "scale_bias": bell_draw(splits[20], (2 * D,), 1.0, 4.0),
        "zero_bias": bell_draw(splits[21], (2 * D,), 1.0, 4.0),
        "token_projection": bell_draw(splits[22], (D, 4 * D), D ** -0.5, 0.21875, ((0, 4),)),
        "token_output": bell_draw(splits[23], (D, D), (D // 16) ** -0.5, 0.875, ((0, 4),)),
        "token_pair_weight": bell_draw(splits[24], (CZ, H), CZ ** -0.5, 0.5),
        "token_up_weight": bell_draw(splits[25], (D, 2 * FF), D ** -0.5, 0.21875, ((0, 4),)),
        "token_down_weight": bell_draw(splits[26], (FF, D), FF ** -0.5, 0.15625, ((0, 4),)),
    }


HIGHEST = lax.Precision.HIGHEST

@jax.custom_vjp
def low(v):
    return lax.optimization_barrier(v.astype(jnp.bfloat16)).astype(jnp.float32)

@jax.custom_vjp
def low_back(v):
    return v

def low_keep(v):
    return (low(v), None)

def low_pass(kept, grad):
    return (grad,)

def back_keep(v):
    return (v, None)

def back_low(kept, grad):
    return (low(grad),)
low.defvjp(low_keep, low_pass)
low_back.defvjp(back_keep, back_low)

def both_round(values):
    return low(low_back(values))

def layer_norm(values):
    centred = values - lax.optimization_barrier(jnp.mean(values, axis=-1, keepdims=True))
    return centred * lax.rsqrt(lax.optimization_barrier(jnp.mean(centred * centred, axis=-1, keepdims=True)) + 1e-05)

def matmul(left_side, right_side):
    return jnp.matmul(left_side, right_side, precision=HIGHEST)

def noise_weight(noise_bin):
    sigma_level = 0.5 * jnp.exp(noise_bin.astype(jnp.float32) * (math.log(8.0) / (NBIN - 1)))
    return 1.0 + 1.0 / (sigma_level * sigma_level)

def conditioning(cond_proj, scale_bias, zero_bias, width):
    return (jax.nn.sigmoid(cond_proj[:, :width] + scale_bias[:width]), cond_proj[:, width:2 * width], jax.nn.sigmoid(cond_proj[:, 2 * width:3 * width] + zero_bias[:width]), jax.nn.sigmoid(cond_proj[:, 3 * width:4 * width] + scale_bias[width:]), cond_proj[:, 4 * width:5 * width], jax.nn.sigmoid(cond_proj[:, 5 * width:] + zero_bias[width:]))

def transition(stream, scale_gate, shift_part, zero_gate, up_weight, down_weight, hidden_width):
    entering = low(layer_norm(stream) * scale_gate + shift_part)
    gate_up = both_round(matmul(entering, up_weight))
    hidden = low(jax.nn.silu(gate_up[:, :hidden_width]) * gate_up[:, hidden_width:])
    return stream + zero_gate * low_back(matmul(hidden, down_weight))

def atom_layer(atom_rows, atom_cond_rows, atom_bias, key_index, key_valid, atom_cond_weight, atom_scale_bias, atom_zero_bias, projection, output_weight, up_weight, down_weight):
    cond_proj = both_round(matmul(low(layer_norm(atom_cond_rows)), atom_cond_weight))
    scale_a, shift_a, zero_a, scale_t, shift_t, zero_t = conditioning(cond_proj, atom_scale_bias, atom_zero_bias, DA)
    entering = low(layer_norm(atom_rows) * scale_a + shift_a)
    projected = both_round(matmul(entering, projection))
    queries = projected[:, :DA].reshape(NWIN, WQ, HA, DHA)
    windowed = projected[key_index.reshape(-1), DA:3 * DA].reshape(NWIN, WK, 2, HA, DHA)
    gate_part = projected[:, 3 * DA:].reshape(NWIN, WQ, HA, DHA)
    scores = low_back(jnp.einsum('wqhe,wkhe->whqk', queries, windowed[:, :, 0], precision=HIGHEST) * DHA ** (-0.5) + atom_bias)
    scores = jnp.where(key_valid[:, None, None, :], scores, -1000000000.0)
    probability = low(jax.nn.softmax(scores, axis=-1))
    attended = low_back(jnp.einsum('whqk,wkhe->wqhe', probability, windowed[:, :, 1], precision=HIGHEST))
    gated = low(attended * jax.nn.sigmoid(gate_part)).reshape(NA, DA)
    middle = atom_rows + zero_a * low_back(matmul(gated, output_weight))
    return transition(middle, scale_t, shift_t, zero_t, up_weight, down_weight, FFA)

def token_layer(token_start, cond_rows, token_bias, cond_weight, scale_bias, zero_bias, projection, output_weight, up_weight, down_weight):
    cond_proj = both_round(matmul(low(layer_norm(cond_rows)), cond_weight))
    scale_a, shift_a, zero_a, scale_t, shift_t, zero_t = conditioning(cond_proj, scale_bias, zero_bias, D)
    entering = low(layer_norm(token_start) * scale_a + shift_a)
    projected = both_round(matmul(entering, projection)).reshape(NT, H, 4 * DH)
    queries = projected[:, :, :DH]
    keys_part = projected[:, :, DH:2 * DH]
    values_part = projected[:, :, 2 * DH:3 * DH]
    gate_part = projected[:, :, 3 * DH:]
    scores = low_back(jnp.einsum('qhe,khe->hqk', queries, keys_part, precision=HIGHEST) * DH ** (-0.5) + token_bias)
    probability = low(jax.nn.softmax(scores, axis=-1))
    attended = low_back(jnp.einsum('hqk,khe->qhe', probability, values_part, precision=HIGHEST))
    gated = both_round(attended * jax.nn.sigmoid(gate_part)).reshape(NT, D)
    middle = token_start + zero_a * low_back(matmul(gated, output_weight))
    return transition(middle, scale_t, shift_t, zero_t, up_weight, down_weight, FF)

def full_forward(values, key_index, key_valid, atom_token, counts):
    atom_rows, atom_conds, token_rows, cond_rows, atom_pair, token_pair, atom_cond_weight, atom_scale_bias, atom_zero_bias, atom_proj, atom_out_weight, atom_pair_weight, atom_up, atom_down, pool_weight, cond_weight, scale_bias, zero_bias, token_proj, token_out_weight, token_pair_weight, token_up, token_down = values
    pair_norm = layer_norm(atom_pair.reshape(NWIN, WQ, WK, CP))
    atom_bias = jnp.einsum('wqkc,ch->whqk', pair_norm, atom_pair_weight, precision=HIGHEST)
    token_bias = both_round(jnp.einsum('rkc,ch->hrk', low(layer_norm(token_pair)), token_pair_weight, precision=HIGHEST))

    def one_sample(atoms_one, atom_cond_one, tokens_one, cond_one):
        final_atoms = atom_layer(atoms_one, atom_cond_one, atom_bias, key_index, key_valid, atom_cond_weight, atom_scale_bias, atom_zero_bias, atom_proj, atom_out_weight, atom_up, atom_down)
        pooled = jax.ops.segment_sum(final_atoms, atom_token, NT) / counts[:, None]
        token_start = tokens_one + low_back(matmul(low(pooled), pool_weight))
        return token_layer(token_start, cond_one, token_bias, cond_weight, scale_bias, zero_bias, token_proj, token_out_weight, token_up, token_down)
    group_size = 8 if SAMPLES % 8 == 0 else 1

    def scan_step(carry_value, batch_rows):
        return (carry_value, jax.vmap(one_sample)(batch_rows[0], batch_rows[1], batch_rows[2], batch_rows[3]))
    stacked = (atom_rows.reshape(SAMPLES // group_size, group_size, NA, DA), atom_conds.reshape(SAMPLES // group_size, group_size, NA, DA), token_rows.reshape(SAMPLES // group_size, group_size, NT, D), cond_rows.reshape(SAMPLES // group_size, group_size, NT, CS))
    unused, outputs = lax.scan(jax.checkpoint(scan_step), jnp.zeros((), jnp.float32), stacked)
    return outputs.reshape(SAMPLES, NT, D)

def reference(atom_single, atom_cond, token_single, token_cond, atom_pair, token_pair, atom_token, window_shift, noise_bin, out_cotangent, atom_cond_weight, atom_scale_bias, atom_zero_bias, atom_projection, atom_output, atom_pair_weight, atom_up_weight, atom_down_weight, pool_weight, cond_weight, scale_bias, zero_bias, token_projection, token_output, token_pair_weight, token_up_weight, token_down_weight):
    floats = tuple((array.astype(jnp.float32) for array in (atom_single, atom_cond, token_single, token_cond, atom_pair, token_pair, atom_cond_weight, atom_scale_bias, atom_zero_bias, atom_projection, atom_output, atom_pair_weight, atom_up_weight, atom_down_weight, pool_weight, cond_weight, scale_bias, zero_bias, token_projection, token_output, token_pair_weight, token_up_weight, token_down_weight)))
    first_key = jnp.arange(NWIN, dtype=jnp.int32) * WQ - (WK - WQ) // 2 + window_shift
    key_pos = first_key[:, None] + jnp.arange(WK, dtype=jnp.int32)[None, :]
    key_valid = (key_pos >= 0) & (key_pos < NA)
    key_index = jnp.clip(key_pos, 0, NA - 1).astype(jnp.int32)
    counts = jax.ops.segment_sum(jnp.ones((NA,), jnp.float32), atom_token, NT)

    def forward(*values):
        return full_forward(values, key_index, key_valid, atom_token, counts)
    output, pullback = jax.vjp(forward, *floats)
    loss_weight = noise_weight(noise_bin)
    gradients = pullback(out_cotangent.astype(jnp.float32) * loss_weight[:, None, None])
    return (output.astype(jnp.bfloat16), gradients[0], gradients[1], gradients[2], gradients[3], gradients[4], gradients[5], gradients[6], gradients[7], gradients[8], gradients[9], gradients[10], gradients[11], gradients[12], gradients[13], gradients[14], gradients[15], gradients[16], gradients[17], gradients[18], gradients[19], gradients[20], gradients[21], gradients[22])
```

```python
import math

import jax
import jax.numpy as jnp
from jax import lax
from jax.experimental import pallas as pl
from jax.experimental.pallas import tpu as pltpu
from jax.sharding import PartitionSpec as P

D = 768
H = 16
DH = 48
FF = 1536
CS = 384
DA = 128
HA = 4
DHA = 32
FFA = 256
CP = 16
WQ = 32
WK = 128
NBIN = 64

MARGIN = WK // 2
CW = 4
ROWS_Q = CW * WQ
LANES = 256

F32 = jnp.float32
BF16 = jnp.bfloat16


def struct(shape, dtype):
    return jax.ShapeDtypeStruct(shape, dtype)


def norm_rows(values):
    centred = values - jnp.mean(values, axis=-1, keepdims=True)
    inverse = lax.rsqrt(jnp.mean(centred * centred, axis=-1, keepdims=True) + 1e-05)
    return (centred * inverse, inverse)


def norm_back(grad_normed, normed, inverse):
    mean_grad = jnp.mean(grad_normed, axis=-1, keepdims=True)
    mean_cross = jnp.mean(grad_normed * normed, axis=-1, keepdims=True)
    return inverse * (grad_normed - mean_grad - normed * mean_cross)


def to_low(values):
    return values.astype(BF16)


def sigmoid(values):
    return jax.nn.sigmoid(values)


def contract(left_side, right_side, left_dim, right_dim):
    return lax.dot_general(
        left_side,
        right_side,
        (((left_dim,), (right_dim,)), ((), ())),
        preferred_element_type=F32,
    )


def product(left_side, right_side):
    return contract(left_side, right_side, 1, 0)


def product_left(left_side, right_side):
    return contract(left_side, right_side, 0, 0)


def product_right(left_side, right_side):
    return contract(left_side, right_side, 1, 1)


def split_low(values):
    high = to_low(values)
    return high, to_low(values - high.astype(F32))


def noise_weight(noise_bin):
    sigma_level = 0.5 * jnp.exp(noise_bin.astype(F32) * (math.log(8.0) / (NBIN - 1)))
    return 1.0 + 1.0 / (sigma_level * sigma_level)


def merge_rows(block):
    return block.reshape(block.shape[0] * block.shape[1], block.shape[2])


def eight_sums(values):
    rows, width = values.shape
    return jnp.sum(values.reshape(rows // 8, 8, width), axis=0)


def whole(shape):
    zeros = (0,) * len(shape)
    return pl.BlockSpec(shape, lambda *_: zeros)


def params(**settings):
    return pltpu.CompilerParams(vmem_limit_bytes=56 * 1024 * 1024, **settings)


def pair_slabs(x_ref, spread_ref):
    spread = spread_ref[...]
    for slab in range(x_ref.shape[1] // LANES):
        lanes = slice(slab * LANES, (slab + 1) * LANES)
        x = x_ref[:, lanes]
        centred = x.astype(F32) - product(x, spread)
        square_high, square_low = split_low(centred * centred)
        variance = product(square_high, spread) + product(square_low, spread)
        inverse = lax.rsqrt(variance + 1e-05)
        yield lanes, centred * inverse, inverse


def pair_forward_kernel(x_ref, spread_ref, weight_ref, bias_ref):
    total = None
    for lanes, normed, _ in pair_slabs(x_ref, spread_ref):
        term = product(to_low(normed), weight_ref[lanes, :])
        total = term if total is None else total + term
    for window in range(bias_ref.shape[0]):
        for head in range(HA):
            bias_ref[window, head * WQ : (head + 1) * WQ, :] = total[
                window * WQ : (window + 1) * WQ, head * WK : (head + 1) * WK
            ]


def pair_forward(pair_rows, spread, weight):
    rows = pair_rows.shape[0]
    step = min(256, rows)
    windows = step // WQ
    return pl.pallas_call(
        pair_forward_kernel,
        grid=(rows // step,),
        in_specs=[
            pl.BlockSpec((step, WK * CP), lambda i: (i, 0)),
            whole(spread.shape),
            whole(weight.shape),
        ],
        out_specs=pl.BlockSpec((windows, HA * WQ, WK), lambda i: (i, 0, 0)),
        out_shape=struct((rows // WQ, HA * WQ, WK), F32),
        compiler_params=params(),
        name="pair_forward",
    )(pair_rows, spread, weight)


def pair_backward_kernel(x_ref, grad_ref, spread_ref, expand_ref, weight_ref, out_ref, sums_ref):
    @pl.when(pl.program_id(0) == 0)
    def _():
        sums_ref[...] = jnp.zeros_like(sums_ref)

    spread = spread_ref[...]
    heads = [
        jnp.concatenate(
            [grad_ref[w, h * WQ : (h + 1) * WQ, :] for w in range(grad_ref.shape[0])], axis=0
        )
        for h in range(HA)
    ]
    for lanes, normed, inverse in pair_slabs(x_ref, spread_ref):
        grad_normed = None
        for head in range(HA):
            wide = product(heads[head], expand_ref[:, lanes])
            sums_ref[head * 8 : (head + 1) * 8, lanes] += eight_sums(wide * normed)
            term = wide * weight_ref[head : head + 1, lanes]
            grad_normed = term if grad_normed is None else grad_normed + term
        mean_grad = product(to_low(grad_normed), spread)
        mean_cross = product(to_low(grad_normed * normed), spread)
        out_ref[:, lanes] = inverse * (grad_normed - mean_grad - normed * mean_cross)


def pair_backward(pair_rows, grad_bias, spread, expand, weight_rows):
    rows = pair_rows.shape[0]
    step = min(256, rows)
    windows = step // WQ
    wide = WK * CP
    return pl.pallas_call(
        pair_backward_kernel,
        grid=(rows // step,),
        in_specs=[
            pl.BlockSpec((step, wide), lambda i: (i, 0)),
            pl.BlockSpec((windows, HA * WQ, WK), lambda i: (i, 0, 0)),
            whole(spread.shape),
            whole(expand.shape),
            whole(weight_rows.shape),
        ],
        out_specs=[
            pl.BlockSpec((step, wide), lambda i: (i, 0)),
            whole((HA * 8, wide)),
        ],
        out_shape=[struct((rows, wide), F32), struct((HA * 8, wide), F32)],
        compiler_params=params(),
        name="pair_backward",
    )(pair_rows, grad_bias, spread, expand, weight_rows)


def atom_entry(single, cond_proj, scale_bias):
    normed, inverse = norm_rows(single)
    scale = sigmoid(cond_proj[:, :DA] + scale_bias[:, :DA])
    return normed, inverse, scale, to_low(normed * scale + cond_proj[:, DA : 2 * DA])


def atom_first_kernel(
    single_ref, cond_ref, cond_weight_ref, scale_ref, proj_weight_ref,
    query_ref, keyval_ref, gate_ref, cond_proj_ref,
):
    samples, rows, _ = single_ref.shape
    cond_low = to_low(norm_rows(merge_rows(cond_ref[...]).astype(F32))[0])
    cond_proj = to_low(product(cond_low, cond_weight_ref[...]))
    cond_proj_ref[...] = cond_proj.reshape(cond_proj_ref.shape)
    single = merge_rows(single_ref[...]).astype(F32)
    entering = atom_entry(single, cond_proj.astype(F32), scale_ref[...])[3]
    projected = to_low(product(entering, proj_weight_ref[...]))
    query_ref[...] = projected[:, :DA].reshape(query_ref.shape)
    keyval_ref[...] = projected[:, DA : 3 * DA].reshape(keyval_ref.shape)
    gate_ref[...] = projected[:, 3 * DA :].reshape(gate_ref.shape)


def atom_first(single, cond, cond_weight, scale_bias, proj_weight):
    samples, atoms, _ = single.shape
    step = min(256, atoms)

    def rows(width):
        return pl.BlockSpec((samples, step, width), lambda i: (0, i, 0))

    widths = (DA, 2 * DA, DA, 6 * DA)
    return pl.pallas_call(
        atom_first_kernel,
        grid=(atoms // step,),
        in_specs=[
            rows(DA), rows(DA), whole(cond_weight.shape), whole(scale_bias.shape),
            whole(proj_weight.shape),
        ],
        out_specs=[rows(width) for width in widths],
        out_shape=[struct((samples, atoms, width), BF16) for width in widths],
        compiler_params=params(),
        name="atom_first",
    )(single, cond, cond_weight, scale_bias, proj_weight)


def wide_shape(extended):
    samples, rows, width = extended.shape
    return (samples, rows + 8, width)


def window_load(ref, sample, start):
    rest = lax.rem(start, 8)
    aligned = pl.multiple_of(start - rest, 8)
    block = ref[sample, pl.ds(aligned, WK + 8), :]
    return pltpu.roll(block, lax.rem(WK + 8 - rest, WK + 8), 0)[:WK]


def window_add(ref, sample, start, values):
    rest = lax.rem(start, 8)
    aligned = pl.multiple_of(start - rest, 8)
    padded = jnp.concatenate([values, jnp.zeros((8, values.shape[1]), values.dtype)], axis=0)
    ref[sample, pl.ds(aligned, WK + 8), :] += pltpu.roll(padded, rest, 0)


def head_masks():
    row_head = lax.broadcasted_iota(jnp.int32, (HA * WQ, DA), 0) // WQ
    lane_head = lax.broadcasted_iota(jnp.int32, (HA * WQ, DA), 1) // DHA
    return row_head == lane_head


def stack_heads(rows, mask):
    wide = jnp.concatenate([rows] * HA, axis=0)
    return jnp.where(mask, wide, jnp.zeros_like(wide))


def fold_heads(stacked, mask):
    kept = jnp.where(mask, stacked, 0.0)
    total = kept[:WQ]
    for head in range(1, HA):
        total = total + kept[head * WQ : (head + 1) * WQ]
    return total


def atom_conditions(cond_proj, scale_bias, zero_bias):
    return (
        sigmoid(cond_proj[:, 2 * DA : 3 * DA] + zero_bias[:, :DA]),
        sigmoid(cond_proj[:, 3 * DA : 4 * DA] + scale_bias[:, DA:]),
        cond_proj[:, 4 * DA : 5 * DA],
        sigmoid(cond_proj[:, 5 * DA :] + zero_bias[:, DA:]),
    )


def member_rows(token_ref, tokens):
    ids = lax.broadcasted_iota(jnp.int32, (tokens, ROWS_Q), 0)
    return ids == jnp.broadcast_to(token_ref[...], (tokens, ROWS_Q))


def atom_second_kernel(
    atoms_all, starts_ref, query_ref, gate_ref, cond_proj_ref, single_ref, extended_ref, bias_ref,
    token_ref, scale_ref, zero_ref, out_weight_ref, up_ref, down_ref,
    prob_ref, gated_ref, middle_ref, pooled_ref, counts_ref, wide_ref,
):
    step = pl.program_id(0)
    samples = query_ref.shape[0]
    tokens = pooled_ref.shape[1]

    @pl.when(step == 0)
    def _():
        wide_ref[:, : extended_ref.shape[1], :] = extended_ref[...].astype(F32)
        pooled_ref[...] = jnp.zeros_like(pooled_ref)
        counts_ref[...] = jnp.zeros_like(counts_ref)

    mask = head_masks()
    lane = lax.broadcasted_iota(jnp.int32, (1, WK), 1)
    pieces = []
    for sample in range(samples):
        for window in range(CW):
            start = starts_ref[0, step * CW + window]
            position = starts_ref[1, step * CW + window] + lane
            valid = (position >= 0) & (position < atoms_all)
            keyval = window_load(wide_ref, sample, start)
            key = to_low(keyval[:, :DA])
            value = to_low(keyval[:, DA:])
            query = stack_heads(query_ref[sample, window * WQ : (window + 1) * WQ, :], mask)
            scores = product_right(query, key) * DHA ** (-0.5) + bias_ref[window]
            scores = jnp.where(valid, scores, -1000000000.0)
            exponent = jnp.exp(scores - jnp.max(scores, axis=-1, keepdims=True))
            prob = to_low(exponent / jnp.sum(exponent, axis=-1, keepdims=True))
            prob_ref[sample, window] = prob
            pieces.append(fold_heads(product(prob, value), mask))
    attended = jnp.concatenate(pieces, axis=0)
    gate = merge_rows(gate_ref[...]).astype(F32)
    gated = to_low(attended * sigmoid(gate))
    gated_ref[...] = gated.reshape(gated_ref.shape)
    cond_proj = merge_rows(cond_proj_ref[...]).astype(F32)
    zero_a, scale_t, shift_t, zero_t = atom_conditions(cond_proj, scale_ref[...], zero_ref[...])
    single = merge_rows(single_ref[...]).astype(F32)
    middle = single + zero_a * product(gated, out_weight_ref[...])
    middle_ref[...] = middle.reshape(middle_ref.shape)
    entering = to_low(norm_rows(middle)[0] * scale_t + shift_t)
    gate_up = to_low(product(entering, up_ref[...])).astype(F32)
    hidden = to_low(jax.nn.silu(gate_up[:, :FFA]) * gate_up[:, FFA:])
    final = middle + zero_t * product(hidden, down_ref[...])
    member = member_rows(token_ref, tokens)
    member_low = member.astype(F32).astype(BF16)
    counts_ref[...] += jnp.broadcast_to(
        jnp.sum(member.astype(F32), axis=1, keepdims=True), counts_ref.shape
    )
    high, rest = split_low(final)
    for sample in range(samples):
        part = slice(sample * ROWS_Q, (sample + 1) * ROWS_Q)
        pooled_ref[sample] += product(member_low, high[part]) + product(member_low, rest[part])

    @pl.when(step == pl.num_programs(0) - 1)
    def _():
        for sample in range(samples):
            pooled_ref[sample] = pooled_ref[sample] / counts_ref[...]


def atom_second(
    atoms_all, starts, query, gate, cond_proj, single, extended, bias, token_row,
    scale_bias, zero_bias, out_weight, up_weight, down_weight, tokens,
):
    samples, atoms, _ = query.shape

    def rows(width):
        return pl.BlockSpec((samples, ROWS_Q, width), lambda i, s: (0, i, 0))

    def kernel(*refs):
        atom_second_kernel(atoms_all, *refs)

    return pl.pallas_call(
        kernel,
        grid_spec=pltpu.PrefetchScalarGridSpec(
            num_scalar_prefetch=1,
            grid=(atoms // ROWS_Q,),
            in_specs=[
                rows(DA), rows(DA), rows(6 * DA), rows(DA), whole(extended.shape),
                pl.BlockSpec((CW, HA * WQ, WK), lambda i, s: (i, 0, 0)),
                pl.BlockSpec((1, ROWS_Q), lambda i, s: (0, i)),
                whole(scale_bias.shape), whole(zero_bias.shape), whole(out_weight.shape),
                whole(up_weight.shape), whole(down_weight.shape),
            ],
            out_specs=[
                pl.BlockSpec((samples, CW, HA * WQ, WK), lambda i, s: (0, i, 0, 0)),
                rows(DA), rows(DA), whole((samples, tokens, DA)), whole((tokens, DA)),
            ],
            scratch_shapes=[pltpu.VMEM(wide_shape(extended), F32)],
        ),
        out_shape=[
            struct((samples, atoms // WQ, HA * WQ, WK), BF16),
            struct((samples, atoms, DA), BF16),
            struct((samples, atoms, DA), F32),
            struct((samples, tokens, DA), F32),
            struct((tokens, DA), F32),
        ],
        compiler_params=params(),
        name="atom_second",
    )(
        starts, query, gate, cond_proj, single, extended, bias, token_row, scale_bias, zero_bias,
        out_weight, up_weight, down_weight,
    )


def atom_third_kernel(
    starts_ref, query_ref, gate_ref, cond_proj_ref, extended_ref, prob_ref, gated_ref, middle_ref,
    pooled_ref, token_ref, scale_ref, zero_ref, out_weight_ref, up_ref, down_ref,
    grad_middle_ref, grad_query_ref, grad_gate_ref, grad_ext_ref, grad_bias_ref, grad_cond_ref,
    grad_out_ref, grad_up_ref, grad_down_ref, sums_ref, wide_ref,
):
    step = pl.program_id(0)
    samples = query_ref.shape[0]
    tokens = pooled_ref.shape[1]

    @pl.when(step == 0)
    def _():
        wide_ref[:, : extended_ref.shape[1], :] = extended_ref[...].astype(F32)
        grad_ext_ref[...] = jnp.zeros_like(grad_ext_ref)
        grad_out_ref[...] = jnp.zeros_like(grad_out_ref)
        grad_up_ref[...] = jnp.zeros_like(grad_up_ref)
        grad_down_ref[...] = jnp.zeros_like(grad_down_ref)
        sums_ref[...] = jnp.zeros_like(sums_ref)

    member = member_rows(token_ref, tokens).astype(F32).astype(BF16)
    grads = []
    for sample in range(samples):
        high, rest = split_low(pooled_ref[sample])
        grads.append(product_left(member, high) + product_left(member, rest))
    grad_stream = jnp.concatenate(grads, axis=0)

    cond_proj = merge_rows(cond_proj_ref[...]).astype(F32)
    zero_a, scale_t, shift_t, zero_t = atom_conditions(cond_proj, scale_ref[...], zero_ref[...])
    normed, inverse = norm_rows(merge_rows(middle_ref[...]))
    entering = to_low(normed * scale_t + shift_t)
    gate_up = to_low(product(entering, up_ref[...])).astype(F32)
    gate_part = gate_up[:, :FFA]
    up_part = gate_up[:, FFA:]
    sig = sigmoid(gate_part)
    silu = gate_part * sig
    hidden = to_low(silu * up_part)
    branch = product(hidden, down_ref[...])
    grad_branch = to_low(grad_stream * zero_t)
    grad_zero_t = grad_stream * branch * zero_t * (1.0 - zero_t)
    grad_down_ref[...] += product_left(hidden, grad_branch)
    grad_hidden = product_right(grad_branch, down_ref[...])
    grad_gate_up = to_low(
        jnp.concatenate(
            [
                grad_hidden * up_part * (sig * (1.0 + gate_part * (1.0 - sig))),
                grad_hidden * silu,
            ],
            axis=1,
        )
    )
    grad_up_ref[...] += product_left(entering, grad_gate_up)
    grad_entering = product_right(grad_gate_up, up_ref[...])
    grad_scale_t = grad_entering * normed * scale_t * (1.0 - scale_t)
    grad_middle = grad_stream + norm_back(grad_entering * scale_t, normed, inverse)
    grad_middle_ref[...] = grad_middle.reshape(grad_middle_ref.shape)

    gated = merge_rows(gated_ref[...])
    branch_a = product(gated, out_weight_ref[...])
    grad_zero_a = grad_middle * branch_a * zero_a * (1.0 - zero_a)
    grad_branch_a = to_low(grad_middle * zero_a)
    grad_out_ref[...] += product_left(gated, grad_branch_a)
    grad_gated = product_right(grad_branch_a, out_weight_ref[...])
    gate_sig = sigmoid(merge_rows(gate_ref[...]).astype(F32))
    grad_gate = grad_gated * gated.astype(F32) * (1.0 - gate_sig)
    grad_gate_ref[...] = to_low(grad_gate).reshape(grad_gate_ref.shape)
    grad_attended = to_low(grad_gated * gate_sig)

    grad_cond_ref[...] = to_low(
        jnp.concatenate([grad_zero_a, grad_scale_t, grad_entering, grad_zero_t], axis=1)
    ).reshape(grad_cond_ref.shape)
    sums_ref[:, :DA] += eight_sums(grad_zero_a)
    sums_ref[:, DA : 2 * DA] += eight_sums(grad_scale_t)
    sums_ref[:, 2 * DA :] += eight_sums(grad_zero_t)

    mask = head_masks()
    grad_bias = [None] * CW
    for sample in range(samples):
        for window in range(CW):
            start = starts_ref[0, step * CW + window]
            first = sample * ROWS_Q + window * WQ
            keyval = window_load(wide_ref, sample, start)
            key = to_low(keyval[:, :DA])
            value = to_low(keyval[:, DA:])
            query = stack_heads(query_ref[sample, window * WQ : (window + 1) * WQ, :], mask)
            grad_wide = stack_heads(grad_attended[first : first + WQ], mask)
            prob = prob_ref[sample, window]
            prob_wide = prob.astype(F32)
            grad_prob = product_right(grad_wide, value)
            inner = jnp.sum(prob_wide * grad_prob, axis=-1, keepdims=True)
            grad_scores = to_low(prob_wide * (grad_prob - inner))
            wide = grad_scores.astype(F32)
            grad_bias[window] = wide if sample == 0 else grad_bias[window] + wide
            grad_query = fold_heads(product(grad_scores, key), mask) * DHA ** (-0.5)
            grad_query_ref[sample, window * WQ : (window + 1) * WQ, :] = to_low(grad_query)
            grad_key = product_left(grad_scores, query) * DHA ** (-0.5)
            grad_value = product_left(prob, grad_wide)
            window_add(
                grad_ext_ref, sample, start, jnp.concatenate([grad_key, grad_value], axis=1)
            )
    for window in range(CW):
        grad_bias_ref[window] = to_low(grad_bias[window])


def atom_third(
    starts, query, gate, cond_proj, extended, prob, gated, middle, grad_pooled, token_row,
    scale_bias, zero_bias, out_weight, up_weight, down_weight,
):
    samples, atoms, _ = query.shape

    def rows(width):
        return pl.BlockSpec((samples, ROWS_Q, width), lambda i, s: (0, i, 0))

    windows = pl.BlockSpec((CW, HA * WQ, WK), lambda i, s: (i, 0, 0))
    return pl.pallas_call(
        atom_third_kernel,
        grid_spec=pltpu.PrefetchScalarGridSpec(
            num_scalar_prefetch=1,
            grid=(atoms // ROWS_Q,),
            in_specs=[
                rows(DA), rows(DA), rows(6 * DA), whole(extended.shape),
                pl.BlockSpec((samples, CW, HA * WQ, WK), lambda i, s: (0, i, 0, 0)),
                rows(DA), rows(DA), whole(grad_pooled.shape),
                pl.BlockSpec((1, ROWS_Q), lambda i, s: (0, i)),
                whole(scale_bias.shape), whole(zero_bias.shape), whole(out_weight.shape),
                whole(up_weight.shape), whole(down_weight.shape),
            ],
            out_specs=[
                rows(DA), rows(DA), rows(DA), whole(wide_shape(extended)), windows, rows(4 * DA),
                whole(out_weight.shape), whole(up_weight.shape), whole(down_weight.shape),
                whole((8, 3 * DA)),
            ],
            scratch_shapes=[pltpu.VMEM(wide_shape(extended), F32)],
        ),
        out_shape=[
            struct((samples, atoms, DA), F32),
            struct((samples, atoms, DA), BF16),
            struct((samples, atoms, DA), BF16),
            struct(wide_shape(extended), F32),
            struct((atoms // WQ, HA * WQ, WK), BF16),
            struct((samples, atoms, 4 * DA), BF16),
            struct(out_weight.shape, F32),
            struct(up_weight.shape, F32),
            struct(down_weight.shape, F32),
            struct((8, 3 * DA), F32),
        ],
        compiler_params=params(),
        name="atom_third",
    )(
        starts, query, gate, cond_proj, extended, prob, gated, middle, grad_pooled, token_row,
        scale_bias, zero_bias, out_weight, up_weight, down_weight,
    )


def atom_fourth_kernel(
    grad_query_ref, grad_gate_ref, grad_ext_ref, low_ref, high_ref, grad_middle_ref,
    grad_cond_ref, single_ref, cond_ref, cond_proj_ref, scale_ref, proj_weight_ref,
    cond_weight_ref, grad_atoms_ref, grad_conds_ref, grad_proj_ref, grad_cond_weight_ref, sums_ref,
):
    step = pl.program_id(0)
    last = pl.num_programs(0) - 1
    samples, rows, _ = single_ref.shape

    @pl.when(step == 0)
    def _():
        grad_proj_ref[...] = jnp.zeros_like(grad_proj_ref)
        grad_cond_weight_ref[...] = jnp.zeros_like(grad_cond_weight_ref)
        sums_ref[...] = jnp.zeros_like(sums_ref)

    first = (step == 0).astype(F32)
    final = (step == last).astype(F32)
    blank = jnp.zeros((rows - MARGIN, 2 * DA), F32)
    keyvals = []
    for sample in range(samples):
        own = grad_ext_ref[sample, pl.ds(pl.multiple_of(MARGIN + step * rows, 8), rows), :]
        from_low = jnp.concatenate([low_ref[sample].astype(F32) * first, blank], axis=0)
        from_high = jnp.concatenate([blank, high_ref[sample].astype(F32) * final], axis=0)
        keyvals.append(to_low(own + from_low + from_high))
    grad_projected = jnp.concatenate(
        [
            merge_rows(grad_query_ref[...]),
            jnp.concatenate(keyvals, axis=0),
            merge_rows(grad_gate_ref[...]),
        ],
        axis=1,
    )
    cond_proj = merge_rows(cond_proj_ref[...]).astype(F32)
    single = merge_rows(single_ref[...]).astype(F32)
    normed, inverse, scale, entering = atom_entry(single, cond_proj, scale_ref[...])
    grad_proj_ref[...] += product_left(entering, grad_projected)
    grad_entering = product_right(grad_projected, proj_weight_ref[...])
    grad_scale = grad_entering * normed * scale * (1.0 - scale)
    sums_ref[...] += eight_sums(grad_scale)
    grad_atoms = merge_rows(grad_middle_ref[...]) + norm_back(
        grad_entering * scale, normed, inverse
    )
    grad_atoms_ref[...] = grad_atoms.reshape(grad_atoms_ref.shape)
    grad_cond_proj = jnp.concatenate(
        [to_low(grad_scale), to_low(grad_entering), merge_rows(grad_cond_ref[...])], axis=1
    )
    cond_norm, cond_inverse = norm_rows(merge_rows(cond_ref[...]).astype(F32))
    grad_cond_weight_ref[...] += product_left(to_low(cond_norm), grad_cond_proj)
    grad_conds = norm_back(
        product_right(grad_cond_proj, cond_weight_ref[...]), cond_norm, cond_inverse
    )
    grad_conds_ref[...] = grad_conds.reshape(grad_conds_ref.shape)


def atom_fourth(
    grad_query, grad_gate, grad_ext, low, high, grad_middle, grad_cond, single, cond, cond_proj,
    scale_bias, proj_weight, cond_weight,
):
    samples, atoms, _ = single.shape
    step = min(256, atoms)

    def rows(width):
        return pl.BlockSpec((samples, step, width), lambda i: (0, i, 0))

    return pl.pallas_call(
        atom_fourth_kernel,
        grid=(atoms // step,),
        in_specs=[
            rows(DA), rows(DA), whole(grad_ext.shape), whole(low.shape), whole(high.shape),
            rows(DA), rows(4 * DA), rows(DA), rows(DA), rows(6 * DA), whole(scale_bias.shape),
            whole(proj_weight.shape), whole(cond_weight.shape),
        ],
        out_specs=[
            rows(DA), rows(DA), whole(proj_weight.shape), whole(cond_weight.shape), whole((8, DA)),
        ],
        out_shape=[
            struct((samples, atoms, DA), F32),
            struct((samples, atoms, DA), F32),
            struct(proj_weight.shape, F32),
            struct(cond_weight.shape, F32),
            struct((8, DA), F32),
        ],
        compiler_params=params(),
        name="atom_fourth",
    )(
        grad_query, grad_gate, grad_ext, low, high, grad_middle, grad_cond, single, cond,
        cond_proj, scale_bias, proj_weight, cond_weight,
    )


def joined_tokens(ref):
    return jnp.concatenate([ref[source, 0] for source in range(ref.shape[0])], axis=1)


def attend_forward_kernel(heads_ref, bias_ref, out_ref, prob_ref):
    joined = joined_tokens(heads_ref)
    query = joined[:DH]
    key = joined[DH : 2 * DH]
    value = joined[2 * DH :]
    bias = bias_ref[...]
    bias = bias.reshape(bias.shape[0] * bias.shape[2], bias.shape[3]).astype(F32)
    scores = product_left(key, query) * DH ** (-0.5) + bias
    exponent = jnp.exp(scores - jnp.max(scores, axis=0, keepdims=True))
    prob = to_low(exponent / jnp.sum(exponent, axis=0, keepdims=True))
    prob_ref[0, 0] = prob
    attended = to_low(product(value, prob))
    tokens = out_ref.shape[3]
    for source in range(out_ref.shape[0]):
        out_ref[source, 0] = attended[:, source * tokens : (source + 1) * tokens]


def attend_forward(heads_view, bias_full):
    groups, samples, width, tokens = heads_view.shape
    parts, heads, keys, rows = bias_full.shape
    return pl.pallas_call(
        attend_forward_kernel,
        grid=(heads, samples),
        in_specs=[
            pl.BlockSpec((groups, 1, 3 * DH, tokens), lambda h, s: (0, s, h, 0)),
            pl.BlockSpec((parts, 1, keys, rows), lambda h, s: (0, h, 0, 0)),
        ],
        out_specs=[
            pl.BlockSpec((groups, 1, DH, tokens), lambda h, s: (0, s, h, 0)),
            pl.BlockSpec((1, 1, rows, rows), lambda h, s: (h, s, 0, 0)),
        ],
        out_shape=[
            struct((groups, samples, heads * DH, tokens), BF16),
            struct((heads, samples, rows, rows), BF16),
        ],
        compiler_params=params(),
        name="attend_forward",
    )(heads_view, bias_full)


def attend_backward_kernel(heads_ref, prob_ref, grad_ref, out_ref, bias_ref, total_ref):
    sample = pl.program_id(1)
    joined = joined_tokens(heads_ref)
    query = joined[:DH]
    key = joined[DH : 2 * DH]
    value = joined[2 * DH :]
    grad = joined_tokens(grad_ref)
    prob = prob_ref[0, 0]
    wide = prob.astype(F32)
    grad_value = product_right(grad, prob)
    grad_prob = product_left(value, grad)
    inner = jnp.sum(wide * grad_prob, axis=0, keepdims=True)
    grad_scores = to_low(wide * (grad_prob - inner))
    grad_query = product(key, grad_scores) * DH ** (-0.5)
    grad_key = product_right(query, grad_scores) * DH ** (-0.5)
    stacked = to_low(jnp.concatenate([grad_query, grad_key, grad_value], axis=0))
    tokens = out_ref.shape[3]
    for source in range(out_ref.shape[0]):
        out_ref[source, 0] = stacked[:, source * tokens : (source + 1) * tokens]

    @pl.when(sample == 0)
    def _():
        total_ref[...] = grad_scores.astype(F32)

    @pl.when(sample > 0)
    def _():
        total_ref[...] += grad_scores.astype(F32)

    @pl.when(sample == pl.num_programs(1) - 1)
    def _():
        bias_ref[...] = to_low(total_ref[...]).reshape(bias_ref.shape)


def attend_backward(heads_view, prob, grad_view, parts):
    groups, samples, width, tokens = heads_view.shape
    heads, _, rows, _ = prob.shape
    keys = rows // parts
    return pl.pallas_call(
        attend_backward_kernel,
        grid=(heads, samples),
        in_specs=[
            pl.BlockSpec((groups, 1, 3 * DH, tokens), lambda h, s: (0, s, h, 0)),
            pl.BlockSpec((1, 1, rows, rows), lambda h, s: (h, s, 0, 0)),
            pl.BlockSpec((groups, 1, DH, tokens), lambda h, s: (0, s, h, 0)),
        ],
        out_specs=[
            pl.BlockSpec((groups, 1, 3 * DH, tokens), lambda h, s: (0, s, h, 0)),
            pl.BlockSpec((parts, 1, keys, rows), lambda h, s: (0, h, 0, 0)),
        ],
        out_shape=[
            struct(heads_view.shape, BF16),
            struct((parts, heads, keys, rows), BF16),
        ],
        scratch_shapes=[pltpu.VMEM((rows, rows), F32)],
        compiler_params=params(),
        name="attend_backward",
    )(heads_view, prob, grad_view)


def conditioning(cond_proj, scale_bias, zero_bias, width):
    return (
        sigmoid(cond_proj[:, :width] + scale_bias[:width]),
        cond_proj[:, width : 2 * width],
        sigmoid(cond_proj[:, 2 * width : 3 * width] + zero_bias[:width]),
        sigmoid(cond_proj[:, 3 * width : 4 * width] + scale_bias[width:]),
        cond_proj[:, 4 * width : 5 * width],
        sigmoid(cond_proj[:, 5 * width :] + zero_bias[width:]),
    )


def transition_forward(stream, scale_gate, shift_part, zero_gate, up_weight, down_weight):
    normed, inverse = norm_rows(stream)
    entering = to_low(normed * scale_gate + shift_part)
    gate_up = to_low(product(entering, up_weight))
    gate_part = gate_up[:, :FF].astype(F32)
    up_part = gate_up[:, FF:].astype(F32)
    hidden = to_low(jax.nn.silu(gate_part) * up_part)
    branch = product(hidden, down_weight)
    return (
        stream + zero_gate * branch,
        (normed, inverse, entering, gate_part, up_part, hidden, branch),
    )


def transition_backward(grad_stream, saved_state, scale_gate, zero_gate, up_weight, down_weight):
    normed, inverse, entering, gate_part, up_part, hidden, branch = saved_state
    grad_branch = to_low(grad_stream * zero_gate)
    grad_zero_pre = grad_stream * branch * zero_gate * (1.0 - zero_gate)
    grad_down = summed_product(hidden, grad_branch, 1, 2, 4, 2)
    grad_hidden = product_right(grad_branch, down_weight)
    sigmoid_gate = sigmoid(gate_part)
    grad_gate = grad_hidden * up_part * (sigmoid_gate * (1.0 + gate_part * (1.0 - sigmoid_gate)))
    grad_up_part = grad_hidden * gate_part * sigmoid_gate
    grad_gate_up = to_low(jnp.concatenate([grad_gate, grad_up_part], axis=1))
    grad_up = summed_product(entering, grad_gate_up, 1, 4, 2, 4)
    grad_entering = product_right(grad_gate_up, up_weight)
    grad_scale_pre = grad_entering * normed * scale_gate * (1.0 - scale_gate)
    grad_input = grad_stream + norm_back(grad_entering * scale_gate, normed, inverse)
    return (grad_input, (grad_scale_pre, grad_entering, grad_zero_pre), grad_up, grad_down)


def direct_exchange():
    return lax.axis_size("dp") == 8 and lax.axis_size("seq") == 4


def bit(axis, mask):
    return (lax.axis_index(axis) // mask) % 2


def xor_send(block, axis, mask):
    count = lax.axis_size(axis)
    return lax.ppermute(block, axis, [(i, i ^ mask) for i in range(count)])


def add_low(left_side, right_side):
    return to_low(left_side.astype(F32) + right_side.astype(F32))


def row_half(block, index):
    rows = block.shape[0] // 2
    return lax.dynamic_slice_in_dim(block, index * rows, rows, 0)


def reduce_rows(block, steps):
    for axis, mask in steps:
        mine = bit(axis, mask)
        received = xor_send(row_half(block, 1 - mine), axis, mask)
        block = add_low(row_half(block, mine), received)
    return block


def gather_rows(block, steps):
    for axis, mask in reversed(steps):
        received = xor_send(block, axis, mask)
        block = jnp.where(
            bit(axis, mask) == 0,
            jnp.concatenate([block, received], axis=0),
            jnp.concatenate([received, block], axis=0),
        )
    return block


def sum_quarters(blocks, first, second):
    steps = (("dp", second), ("seq", 1), ("seq", 2))
    near = add_low(blocks[0], xor_send(blocks[2], "dp", 1))
    far = add_low(blocks[1], xor_send(blocks[3], "dp", 1))
    total = add_low(near, xor_send(far, "dp", first))
    own = gather_rows(reduce_rows(total, steps), steps)
    side = xor_send(own, "dp", first)
    return (own, side, xor_send(own, "dp", 1), xor_send(side, "dp", 1))


def sum_halves(blocks, first, second):
    steps = (("dp", first), ("dp", second), ("seq", 1), ("seq", 2))
    total = add_low(blocks[0], xor_send(blocks[1], "dp", 1))
    own = gather_rows(reduce_rows(total, steps), steps)
    return (own, xor_send(own, "dp", 1))


def place_columns_kernel(place_ref, *refs):
    pieces, out_ref = refs[:-1], refs[-1]
    width = pieces[0].shape[1]
    for index, piece in enumerate(pieces):
        column = pl.multiple_of((index ^ place_ref[0]) * width, 128)
        out_ref[:, pl.ds(column, width)] = piece[...].astype(F32)


def place_columns(pieces, place):
    rows, width = pieces[0].shape
    step = rows // 4 if rows >= 512 else rows
    return pl.pallas_call(
        place_columns_kernel,
        grid_spec=pltpu.PrefetchScalarGridSpec(
            num_scalar_prefetch=1,
            grid=(rows // step,),
            in_specs=[pl.BlockSpec((step, width), lambda i, p: (i, 0)) for _ in pieces],
            out_specs=pl.BlockSpec((step, width * len(pieces)), lambda i, p: (i, 0)),
        ),
        out_shape=struct((rows, width * len(pieces)), F32),
        compiler_params=params(),
        name="place_columns",
    )(place.reshape(1).astype(jnp.int32), *pieces)


def summed_product(left_side, right_side, right_dim, count, first, second):
    left_dim = 0
    if left_side.shape[0] != right_side.shape[1 - right_dim]:
        left_dim = 1
    total_width = right_side.shape[right_dim]
    if not direct_exchange():
        full = contract(left_side, right_side, left_dim, 1 - right_dim)
        return lax.psum(to_low(full), ("dp", "seq")).astype(F32)
    width = total_width // count
    place = bit("dp", 1)
    if count == 4:
        place = place * 2 + bit("dp", first)
    blocks = []
    for index in range(count):
        part = lax.dynamic_slice_in_dim(
            right_side, (index ^ place) * width, width, right_dim
        )
        blocks.append(to_low(contract(left_side, part, left_dim, 1 - right_dim)))
    combine = sum_quarters if count == 4 else sum_halves
    return place_columns(combine(blocks, first, second), place)


def summed_array(values, first, second):
    if not direct_exchange():
        return lax.psum(to_low(values), ("dp", "seq")).astype(F32)
    width = values.shape[1] // 4
    place = bit("dp", 1) * 2 + bit("dp", first)
    low = to_low(values)
    blocks = [
        lax.dynamic_slice_in_dim(low, (index ^ place) * width, width, 1) for index in range(4)
    ]
    return place_columns(sum_quarters(blocks, first, second), place)


def summed_rows(values):
    if not direct_exchange():
        return lax.psum(values, "dp")
    steps = (("dp", 1), ("dp", 2), ("dp", 4))
    return gather_rows(reduce_rows(values, steps), steps)


def scattered_rows(values):
    if not direct_exchange():
        return lax.psum_scatter(values, "dp", scatter_dimension=0, tiled=False)
    steps = (("dp", 4), ("dp", 2), ("dp", 1))
    return reduce_rows(values, steps)[0]


PIECE = 384


def place_weights_kernel(shapes, place_ref, *refs):
    count = len(shapes)
    stacks, shards, outs = refs[:8], refs[8 : 8 + count], refs[8 + count :]
    relative = pl.program_id(0) ^ place_ref[1]

    @pl.when(relative == 0)
    def _():
        for shard, out in zip(shards, outs):
            out[...] = shard[...]

    @pl.when(relative != 0)
    def _():
        for index, stack in enumerate(stacks):
            owner = index ^ place_ref[0]
            first = 0
            for (row_parts, rows, width), out in zip(shapes, outs):
                row = pl.multiple_of((owner % row_parts) * rows, 16)
                column = (owner // row_parts) * width
                for offset in range(0, width, PIECE):
                    out[pl.ds(row, rows), pl.ds(pl.multiple_of(column + offset, 128), PIECE)] = (
                        stack[0, first : first + rows, :]
                    )
                    first += rows


def gather_weights(shards, column_parts):
    groups = lax.axis_size("seq")
    if not direct_exchange():
        return tuple(lax.all_gather(shard, "seq", axis=0, tiled=True) for shard in shards)
    place = lax.axis_index("dp")
    shapes, slabs = [], []
    for shard, columns in zip(shards, column_parts):
        row_parts = 8 // columns
        rows, width = shard.shape[0] // row_parts, shard.shape[1] // columns
        shapes.append((row_parts, rows, width))
        piece = lax.dynamic_slice(
            shard, ((place % row_parts) * rows, (place // row_parts) * width), (rows, width)
        )
        slabs += [piece[:, offset : offset + PIECE] for offset in range(0, width, PIECE)]
    slab = jnp.concatenate(slabs, axis=0)
    stack = jnp.stack([xor_send(slab, "seq", mask) for mask in range(1, groups)])
    even = [stack] + [xor_send(stack, "dp", mask) for mask in (2, 4, 6)]
    stacks = []
    for item in even:
        stacks += [item, xor_send(item, "dp", 1)]

    def kernel(*refs):
        place_weights_kernel(shapes, *refs)

    return pl.pallas_call(
        kernel,
        grid_spec=pltpu.PrefetchScalarGridSpec(
            num_scalar_prefetch=1,
            grid=(groups,),
            in_specs=[
                pl.BlockSpec(
                    (1,) + slab.shape, lambda i, p: (jnp.maximum((i ^ p[1]) - 1, 0), 0, 0)
                )
                for _ in stacks
            ]
            + [whole(shard.shape) for shard in shards],
            out_specs=[pl.BlockSpec(shard.shape, lambda i, p: (i, 0)) for shard in shards],
        ),
        out_shape=[
            struct((groups * shard.shape[0], shard.shape[1]), shard.dtype) for shard in shards
        ],
        compiler_params=params(),
        name="place_weights",
    )(jnp.stack([place, lax.axis_index("seq")]).astype(jnp.int32), *stacks, *shards)


def swap(block):
    return lax.all_to_all(block, "seq", split_axis=0, concat_axis=0, tiled=True)


def neighbour_rows(to_next, to_previous):
    count = lax.axis_size("seq")
    forward = [(i, i + 1) for i in range(count - 1)]
    backward = [(i + 1, i) for i in range(count - 1)]
    return (
        lax.ppermute(to_next, "seq", forward),
        lax.ppermute(to_previous, "seq", backward),
    )


def per_device(
    atom_single,
    atom_cond,
    token_single,
    token_cond,
    atom_pair,
    token_pair,
    atom_token,
    window_shift,
    noise_bin,
    out_cotangent,
    atom_cond_weight,
    atom_scale_bias,
    atom_zero_bias,
    atom_projection,
    atom_output,
    atom_pair_weight,
    atom_up_weight,
    atom_down_weight,
    pool_weight,
    cond_weight,
    scale_bias,
    zero_bias,
    token_projection,
    token_output,
    token_pair_weight,
    token_up_weight,
    token_down_weight,
):
    groups = lax.axis_size("seq")
    parts = lax.axis_size("dp")
    place = lax.axis_index("seq")
    samples, atoms_dev, _ = atom_single.shape
    tokens_dev = token_single.shape[1]
    rows_token = samples * tokens_dev
    windows_dev = atoms_dev // WQ
    heads_dev = H // groups
    keys_dev = token_pair.shape[1]
    tokens_all = tokens_dev * groups

    cond_full, projection_full = gather_weights((cond_weight, token_projection), (4, 4))
    output_full, up_full, down_full = gather_weights(
        (token_output, token_up_weight, token_down_weight), (2, 4, 2)
    )

    pair_norm_token, pair_inverse_token = norm_rows(token_pair.astype(F32))
    pair_low = to_low(pair_norm_token)
    bias_local = to_low(
        jnp.einsum("rkc,ch->hkr", pair_low, token_pair_weight, preferred_element_type=F32)
    )
    bias_swapped = swap(bias_local.reshape(groups, heads_dev, keys_dev, tokens_dev))
    bias_heads = bias_swapped.transpose(1, 2, 0, 3).reshape(heads_dev, keys_dev, tokens_all)
    bias_full = lax.all_gather(bias_heads, "dp", axis=0, tiled=False)

    key_lane = jnp.arange(LANES) // CP
    spread = to_low((key_lane[:, None] == key_lane[None, :]).astype(F32) / CP)
    pair_key = jnp.arange(WK * CP) // CP
    expand = to_low(jnp.arange(WK)[:, None] == pair_key[None, :])
    pair_wide = (
        jnp.eye(WK, dtype=BF16)[:, None, None, :] * atom_pair_weight[None, :, :, None]
    ).reshape(WK * CP, HA * WK)
    pair_weight_rows = jnp.tile(atom_pair_weight.astype(F32).T, (1, WK))
    pair_rows = atom_pair.reshape(windows_dev * WQ, WK * CP)
    bias_atom = pair_forward(pair_rows, spread, pair_wide)

    atom_scale = atom_scale_bias.astype(F32).reshape(1, 2 * DA)
    atom_zero = atom_zero_bias.astype(F32).reshape(1, 2 * DA)
    query_atom, keyval_atom, gate_atom, cond_proj_atom = atom_first(
        atom_single, atom_cond, atom_cond_weight, atom_scale, atom_projection
    )
    from_low, from_high = neighbour_rows(
        keyval_atom[:, atoms_dev - MARGIN :], keyval_atom[:, :MARGIN]
    )
    extended = jnp.concatenate([from_low, keyval_atom, from_high], axis=1)
    first_key = jnp.arange(windows_dev, dtype=jnp.int32) * WQ - (WK - WQ) // 2 + window_shift
    starts = jnp.stack([first_key + MARGIN, first_key + place * atoms_dev])
    token_row = (atom_token - place * tokens_dev).reshape(1, atoms_dev)
    prob_atom, gated_atom, middle_atom, pooled, counts = atom_second(
        atoms_dev * groups, starts, query_atom, gate_atom, cond_proj_atom, atom_single, extended,
        bias_atom, token_row, atom_scale, atom_zero, atom_output, atom_up_weight,
        atom_down_weight, tokens_dev,
    )

    pooled_low = to_low(pooled).reshape(rows_token, DA)
    token_start = token_single.astype(F32).reshape(rows_token, D) + product(
        pooled_low, pool_weight
    )
    cond_norm, cond_inverse = norm_rows(token_cond.astype(F32).reshape(rows_token, CS))
    cond_low = to_low(cond_norm)
    cond_proj = to_low(product(cond_low, cond_full)).astype(F32)
    scale_a_tok, shift_a_tok, zero_a_tok, scale_t_tok, shift_t_tok, zero_t_tok = conditioning(
        cond_proj, scale_bias.astype(F32), zero_bias.astype(F32), D
    )
    normed_token, inverse_token = norm_rows(token_start)
    entering_token = to_low(normed_token * scale_a_tok + shift_a_tok)
    projected = to_low(contract(projection_full, entering_token, 0, 1)).reshape(
        groups, heads_dev, 4 * DH, samples, tokens_dev
    )
    heads_view = swap(
        projected[:, :, : 3 * DH]
        .transpose(0, 3, 1, 2, 4)
        .reshape(groups, samples, heads_dev * 3 * DH, tokens_dev)
    )
    gate_sig_token = sigmoid(projected[:, :, 3 * DH :].reshape(D, rows_token).astype(F32))
    attended_swapped, prob_token = attend_forward(heads_view, bias_full)
    attended_token = (
        swap(attended_swapped).transpose(0, 2, 1, 3).reshape(D, rows_token).astype(F32)
    )
    gated_token = to_low(attended_token * gate_sig_token)
    branch_token = product_left(gated_token, output_full)
    middle_token = token_start + zero_a_tok * branch_token
    final_token, saved_token = transition_forward(
        middle_token, scale_t_tok, shift_t_tok, zero_t_tok, up_full, down_full
    )
    block_out = final_token.astype(BF16).reshape(samples, tokens_dev, D)

    loss_weight = noise_weight(noise_bin)
    grad_final = (out_cotangent.astype(F32) * loss_weight[:, None, None]).reshape(rows_token, D)
    grad_middle_token, trans_grads_tok, grad_token_up, grad_token_down = transition_backward(
        grad_final, saved_token, scale_t_tok, zero_t_tok, up_full, down_full
    )
    grad_branch_token = to_low(grad_middle_token * zero_a_tok)
    grad_zero_pre = grad_middle_token * branch_token * zero_a_tok * (1.0 - zero_a_tok)
    grad_token_out = summed_product(gated_token, grad_branch_token, 1, 2, 4, 2)
    grad_gated = to_low(product_right(output_full, grad_branch_token)).astype(F32)
    grad_attended = to_low(grad_gated * gate_sig_token)
    grad_gate_token = to_low(
        grad_gated * attended_token * gate_sig_token * (1.0 - gate_sig_token)
    )
    grad_view = swap(
        grad_attended.reshape(groups, heads_dev * DH, samples, tokens_dev).transpose(0, 2, 1, 3)
    )
    grad_heads, grad_bias = attend_backward(heads_view, prob_token, grad_view, parts)
    grad_rows = (
        swap(grad_heads)
        .transpose(0, 2, 1, 3)
        .reshape(groups, heads_dev, 3 * DH, rows_token)
    )
    grad_projected = jnp.concatenate(
        [grad_rows, grad_gate_token.reshape(groups, heads_dev, DH, rows_token)], axis=2
    ).reshape(4 * D, rows_token)
    grad_token_proj = summed_product(entering_token, grad_projected, 0, 4, 2, 4)
    grad_entering_token = contract(grad_projected, projection_full, 0, 1)
    grad_scale_pre = grad_entering_token * normed_token * scale_a_tok * (1.0 - scale_a_tok)
    grad_cond_proj = to_low(
        jnp.concatenate(
            [
                grad_scale_pre,
                grad_entering_token,
                grad_zero_pre,
                trans_grads_tok[0],
                trans_grads_tok[1],
                trans_grads_tok[2],
            ],
            axis=1,
        )
    )
    grad_cond_full = summed_product(cond_low, grad_cond_proj, 1, 4, 4, 2)
    grad_cond = norm_back(product_right(grad_cond_proj, cond_full), cond_norm, cond_inverse)
    grad_start = grad_middle_token + norm_back(
        grad_entering_token * scale_a_tok, normed_token, inverse_token
    )
    grad_scale_bias = jnp.concatenate(
        [jnp.sum(grad_scale_pre, axis=0), jnp.sum(trans_grads_tok[0], axis=0)]
    )
    grad_zero_bias = jnp.concatenate(
        [jnp.sum(grad_zero_pre, axis=0), jnp.sum(trans_grads_tok[2], axis=0)]
    )
    grad_pool_branch = to_low(grad_start)
    grad_pool = product_left(pooled_low, grad_pool_branch)
    grad_pooled = (
        product_right(grad_pool_branch, pool_weight).reshape(samples, tokens_dev, DA) / counts
    )

    grad_bias_keys = scattered_rows(grad_bias)
    grad_bias_rows = (
        swap(
            grad_bias_keys.reshape(heads_dev, keys_dev, groups, tokens_dev).transpose(2, 0, 1, 3)
        )
        .reshape(H, keys_dev, tokens_dev)
    )
    grad_pair_weight_token = jnp.einsum(
        "rkc,hkr->ch", pair_low, grad_bias_rows, preferred_element_type=F32
    )
    grad_pair_low = jnp.einsum(
        "hkr,ch->rkc", grad_bias_rows, token_pair_weight, preferred_element_type=F32
    )
    grad_token_pair = norm_back(grad_pair_low, pair_norm_token, pair_inverse_token)

    (
        grad_middle_atom, grad_query, grad_gate, grad_ext, grad_bias_atom, grad_cond_atom,
        grad_atom_out, grad_atom_up, grad_atom_down, sums_third,
    ) = atom_third(
        starts, query_atom, gate_atom, cond_proj_atom, extended, prob_atom, gated_atom,
        middle_atom, grad_pooled, token_row, atom_scale, atom_zero, atom_output, atom_up_weight,
        atom_down_weight,
    )
    grad_bias_whole = summed_rows(grad_bias_atom)
    back_low, back_high = neighbour_rows(
        to_low(grad_ext[:, atoms_dev + MARGIN : atoms_dev + 2 * MARGIN]), to_low(grad_ext[:, :MARGIN])
    )
    grad_atoms, grad_atom_conds, grad_atom_proj, grad_atom_cond_weight, sums_fourth = atom_fourth(
        grad_query, grad_gate, grad_ext, back_low, back_high, grad_middle_atom, grad_cond_atom,
        atom_single, atom_cond, cond_proj_atom, atom_scale, atom_projection, atom_cond_weight,
    )
    grad_atom_pair, pair_sums = pair_backward(
        pair_rows, grad_bias_whole, spread, expand, pair_weight_rows
    )
    grad_pair_weight_atom = (
        pair_sums.reshape(HA, 8, WK, CP).sum(axis=(1, 2)).T.reshape(CP * HA) / parts
    )
    sums_third = jnp.sum(sums_third, axis=0)
    grad_atom_scale_bias = jnp.concatenate(
        [jnp.sum(sums_fourth, axis=0), sums_third[DA : 2 * DA]]
    )
    grad_atom_zero_bias = jnp.concatenate([sums_third[:DA], sums_third[2 * DA :]])
    small = jnp.concatenate(
        [
            grad_scale_bias,
            grad_zero_bias,
            grad_atom_scale_bias,
            grad_atom_zero_bias,
            grad_pair_weight_token.reshape(-1),
            grad_pair_weight_atom,
        ]
    )
    small = jnp.pad(small, (0, DA * DA - small.shape[0])).reshape(DA, DA)
    parts_late = (
        grad_pool, grad_atom_cond_weight, grad_atom_proj, grad_atom_out, grad_atom_up,
        grad_atom_down[:DA], grad_atom_down[DA:], small,
    )
    late_sum = summed_array(jnp.concatenate(parts_late, axis=1), 2, 4)
    late = []
    first = 0
    for part in parts_late:
        late.append(late_sum[:, first : first + part.shape[1]])
        first += part.shape[1]
    small = late[7].reshape(-1)
    pieces = []
    first = 0
    for shape in ((2 * D,), (2 * D,), (2 * DA,), (2 * DA,), (128, H), (CP, HA)):
        size = math.prod(shape)
        pieces.append(small[first : first + size].reshape(shape))
        first += size
    return (
        block_out,
        grad_atoms,
        grad_atom_conds,
        grad_start.reshape(samples, tokens_dev, D),
        grad_cond.reshape(samples, tokens_dev, CS),
        grad_atom_pair.reshape(windows_dev, WQ, WK * CP),
        grad_token_pair,
        late[1],
        pieces[2],
        pieces[3],
        late[2],
        late[3],
        pieces[5],
        late[4],
        jnp.concatenate([late[5], late[6]], axis=0),
        late[0],
        grad_cond_full,
        pieces[0],
        pieces[1],
        grad_token_proj,
        grad_token_out,
        pieces[4],
        grad_token_up,
        grad_token_down,
    )


def solution(mesh):
    in_specs = (
        P("dp", "seq", None),
        P("dp", "seq", None),
        P("dp", "seq", None),
        P("dp", "seq", None),
        P("seq", None, None),
        P("seq", "dp", None),
        P("seq"),
        P("seq"),
        P("dp"),
        P("dp", "seq", None),
        P(),
        P(),
        P(),
        P(),
        P(),
        P(),
        P(),
        P(),
        P(),
        P("seq", None),
        P(),
        P(),
        P("seq", None),
        P("seq", None),
        P(),
        P("seq", None),
        P("seq", None),
    )
    out_specs = (
        P("dp", "seq", None),
        P("dp", "seq", None),
        P("dp", "seq", None),
        P("dp", "seq", None),
        P("dp", "seq", None),
        P("seq", None, None),
        P("seq", "dp", None),
    ) + (P(),) * 17
    return jax.shard_map(
        per_device, mesh=mesh, in_specs=in_specs, out_specs=out_specs, check_vma=False
    )
```

```python
import math

import jax
import jax.numpy as jnp
from jax import lax
from jax.experimental import pallas as pl
from jax.experimental.pallas import tpu as pltpu
from jax.sharding import PartitionSpec as P

D = 768
H = 16
DH = 48
FF = 1536
CS = 384
DA = 128
HA = 4
DHA = 32
FFA = 256
CP = 16
WQ = 32
WK = 128
NBIN = 64

MARGIN = WK // 2
CW = 4
ROWS_Q = CW * WQ
LANES = 256

F32 = jnp.float32
BF16 = jnp.bfloat16


def struct(shape, dtype):
    return jax.ShapeDtypeStruct(shape, dtype)


def norm_rows(values):
    centred = values - jnp.mean(values, axis=-1, keepdims=True)
    inverse = lax.rsqrt(jnp.mean(centred * centred, axis=-1, keepdims=True) + 1e-05)
    return (centred * inverse, inverse)


def norm_back(grad_normed, normed, inverse):
    mean_grad = jnp.mean(grad_normed, axis=-1, keepdims=True)
    mean_cross = jnp.mean(grad_normed * normed, axis=-1, keepdims=True)
    return inverse * (grad_normed - mean_grad - normed * mean_cross)


def to_low(values):
    return values.astype(BF16)


def sigmoid(values):
    return jax.nn.sigmoid(values)


def contract(left_side, right_side, left_dim, right_dim):
    return lax.dot_general(
        left_side,
        right_side,
        (((left_dim,), (right_dim,)), ((), ())),
        preferred_element_type=F32,
    )


def product(left_side, right_side):
    return contract(left_side, right_side, 1, 0)


def product_left(left_side, right_side):
    return contract(left_side, right_side, 0, 0)


def product_right(left_side, right_side):
    return contract(left_side, right_side, 1, 1)


def split_low(values):
    high = to_low(values)
    return high, to_low(values - high.astype(F32))


def noise_weight(noise_bin):
    sigma_level = 0.5 * jnp.exp(noise_bin.astype(F32) * (math.log(8.0) / (NBIN - 1)))
    return 1.0 + 1.0 / (sigma_level * sigma_level)


def merge_rows(block):
    return block.reshape(block.shape[0] * block.shape[1], block.shape[2])


def eight_sums(values):
    rows, width = values.shape
    return jnp.sum(values.reshape(rows // 8, 8, width), axis=0)


def whole(shape):
    zeros = (0,) * len(shape)
    return pl.BlockSpec(shape, lambda *_: zeros)


def params(**settings):
    return pltpu.CompilerParams(vmem_limit_bytes=56 * 1024 * 1024, **settings)


def pair_slabs(x_ref, spread_ref):
    spread = spread_ref[...]
    for slab in range(x_ref.shape[1] // LANES):
        lanes = slice(slab * LANES, (slab + 1) * LANES)
        x = x_ref[:, lanes]
        centred = x.astype(F32) - product(x, spread)
        square_high, square_low = split_low(centred * centred)
        variance = product(square_high, spread) + product(square_low, spread)
        inverse = lax.rsqrt(variance + 1e-05)
        yield lanes, centred * inverse, inverse


def pair_forward_kernel(x_ref, spread_ref, weight_ref, bias_ref):
    total = None
    for lanes, normed, _ in pair_slabs(x_ref, spread_ref):
        term = product(to_low(normed), weight_ref[lanes, :])
        total = term if total is None else total + term
    for window in range(bias_ref.shape[0]):
        for head in range(HA):
            bias_ref[window, head * WQ : (head + 1) * WQ, :] = total[
                window * WQ : (window + 1) * WQ, head * WK : (head + 1) * WK
            ]


def pair_forward(pair_rows, spread, weight):
    rows = pair_rows.shape[0]
    step = min(256, rows)
    windows = step // WQ
    return pl.pallas_call(
        pair_forward_kernel,
        grid=(rows // step,),
        in_specs=[
            pl.BlockSpec((step, WK * CP), lambda i: (i, 0)),
            whole(spread.shape),
            whole(weight.shape),
        ],
        out_specs=pl.BlockSpec((windows, HA * WQ, WK), lambda i: (i, 0, 0)),
        out_shape=struct((rows // WQ, HA * WQ, WK), F32),
        compiler_params=params(),
        name="pair_forward",
    )(pair_rows, spread, weight)


def pair_backward_kernel(x_ref, grad_ref, spread_ref, expand_ref, weight_ref, out_ref, sums_ref):
    @pl.when(pl.program_id(0) == 0)
    def _():
        sums_ref[...] = jnp.zeros_like(sums_ref)

    spread = spread_ref[...]
    heads = [
        jnp.concatenate(
            [grad_ref[w, h * WQ : (h + 1) * WQ, :] for w in range(grad_ref.shape[0])], axis=0
        )
        for h in range(HA)
    ]
    for lanes, normed, inverse in pair_slabs(x_ref, spread_ref):
        grad_normed = None
        for head in range(HA):
            wide = product(heads[head], expand_ref[:, lanes])
            sums_ref[head * 8 : (head + 1) * 8, lanes] += eight_sums(wide * normed)
            term = wide * weight_ref[head : head + 1, lanes]
            grad_normed = term if grad_normed is None else grad_normed + term
        mean_grad = product(to_low(grad_normed), spread)
        mean_cross = product(to_low(grad_normed * normed), spread)
        out_ref[:, lanes] = inverse * (grad_normed - mean_grad - normed * mean_cross)


def pair_backward(pair_rows, grad_bias, spread, expand, weight_rows):
    rows = pair_rows.shape[0]
    step = min(256, rows)
    windows = step // WQ
    wide = WK * CP
    return pl.pallas_call(
        pair_backward_kernel,
        grid=(rows // step,),
        in_specs=[
            pl.BlockSpec((step, wide), lambda i: (i, 0)),
            pl.BlockSpec((windows, HA * WQ, WK), lambda i: (i, 0, 0)),
            whole(spread.shape),
            whole(expand.shape),
            whole(weight_rows.shape),
        ],
        out_specs=[
            pl.BlockSpec((step, wide), lambda i: (i, 0)),
            whole((HA * 8, wide)),
        ],
        out_shape=[struct((rows, wide), F32), struct((HA * 8, wide), F32)],
        compiler_params=params(),
        name="pair_backward",
    )(pair_rows, grad_bias, spread, expand, weight_rows)


def atom_entry(single, cond_proj, scale_bias):
    normed, inverse = norm_rows(single)
    scale = sigmoid(cond_proj[:, :DA] + scale_bias[:, :DA])
    return normed, inverse, scale, to_low(normed * scale + cond_proj[:, DA : 2 * DA])


def atom_first_kernel(
    single_ref, cond_ref, cond_weight_ref, scale_ref, proj_weight_ref,
    query_ref, keyval_ref, gate_ref, cond_proj_ref,
):
    samples, rows, _ = single_ref.shape
    cond_low = to_low(norm_rows(merge_rows(cond_ref[...]).astype(F32))[0])
    cond_proj = to_low(product(cond_low, cond_weight_ref[...]))
    cond_proj_ref[...] = cond_proj.reshape(cond_proj_ref.shape)
    single = merge_rows(single_ref[...]).astype(F32)
    entering = atom_entry(single, cond_proj.astype(F32), scale_ref[...])[3]
    projected = to_low(product(entering, proj_weight_ref[...]))
    query_ref[...] = projected[:, :DA].reshape(query_ref.shape)
    keyval_ref[...] = projected[:, DA : 3 * DA].reshape(keyval_ref.shape)
    gate_ref[...] = projected[:, 3 * DA :].reshape(gate_ref.shape)


def atom_first(single, cond, cond_weight, scale_bias, proj_weight):
    samples, atoms, _ = single.shape
    step = min(256, atoms)

    def rows(width):
        return pl.BlockSpec((samples, step, width), lambda i: (0, i, 0))

    widths = (DA, 2 * DA, DA, 6 * DA)
    return pl.pallas_call(
        atom_first_kernel,
        grid=(atoms // step,),
        in_specs=[
            rows(DA), rows(DA), whole(cond_weight.shape), whole(scale_bias.shape),
            whole(proj_weight.shape),
        ],
        out_specs=[rows(width) for width in widths],
        out_shape=[struct((samples, atoms, width), BF16) for width in widths],
        compiler_params=params(),
        name="atom_first",
    )(single, cond, cond_weight, scale_bias, proj_weight)


def wide_shape(extended):
    samples, rows, width = extended.shape
    return (samples, rows + 8, width)


def window_load(ref, sample, start):
    rest = lax.rem(start, 8)
    aligned = pl.multiple_of(start - rest, 8)
    block = ref[sample, pl.ds(aligned, WK + 8), :]
    return pltpu.roll(block, lax.rem(WK + 8 - rest, WK + 8), 0)[:WK]


def window_add(ref, sample, start, values):
    rest = lax.rem(start, 8)
    aligned = pl.multiple_of(start - rest, 8)
    padded = jnp.concatenate([values, jnp.zeros((8, values.shape[1]), values.dtype)], axis=0)
    ref[sample, pl.ds(aligned, WK + 8), :] += pltpu.roll(padded, rest, 0)


def head_masks():
    row_head = lax.broadcasted_iota(jnp.int32, (HA * WQ, DA), 0) // WQ
    lane_head = lax.broadcasted_iota(jnp.int32, (HA * WQ, DA), 1) // DHA
    return row_head == lane_head


def stack_heads(rows, mask):
    wide = jnp.concatenate([rows] * HA, axis=0)
    return jnp.where(mask, wide, jnp.zeros_like(wide))


def fold_heads(stacked, mask):
    kept = jnp.where(mask, stacked, 0.0)
    total = kept[:WQ]
    for head in range(1, HA):
        total = total + kept[head * WQ : (head + 1) * WQ]
    return total


def atom_conditions(cond_proj, scale_bias, zero_bias):
    return (
        sigmoid(cond_proj[:, 2 * DA : 3 * DA] + zero_bias[:, :DA]),
        sigmoid(cond_proj[:, 3 * DA : 4 * DA] + scale_bias[:, DA:]),
        cond_proj[:, 4 * DA : 5 * DA],
        sigmoid(cond_proj[:, 5 * DA :] + zero_bias[:, DA:]),
    )


def member_rows(token_ref, tokens):
    ids = lax.broadcasted_iota(jnp.int32, (tokens, ROWS_Q), 0)
    return ids == jnp.broadcast_to(token_ref[...], (tokens, ROWS_Q))


def atom_second_kernel(
    atoms_all, starts_ref, query_ref, gate_ref, cond_proj_ref, single_ref, extended_ref, bias_ref,
    token_ref, scale_ref, zero_ref, out_weight_ref, up_ref, down_ref,
    prob_ref, gated_ref, middle_ref, pooled_ref, counts_ref, wide_ref,
):
    step = pl.program_id(0)
    samples = query_ref.shape[0]
    tokens = pooled_ref.shape[1]

    @pl.when(step == 0)
    def _():
        wide_ref[:, : extended_ref.shape[1], :] = extended_ref[...].astype(F32)
        pooled_ref[...] = jnp.zeros_like(pooled_ref)
        counts_ref[...] = jnp.zeros_like(counts_ref)

    mask = head_masks()
    lane = lax.broadcasted_iota(jnp.int32, (1, WK), 1)
    pieces = []
    for sample in range(samples):
        for window in range(CW):
            start = starts_ref[0, step * CW + window]
            position = starts_ref[1, step * CW + window] + lane
            valid = (position >= 0) & (position < atoms_all)
            keyval = window_load(wide_ref, sample, start)
            key = to_low(keyval[:, :DA])
            value = to_low(keyval[:, DA:])
            query = stack_heads(query_ref[sample, window * WQ : (window + 1) * WQ, :], mask)
            scores = product_right(query, key) * DHA ** (-0.5) + bias_ref[window]
            scores = jnp.where(valid, scores, -1000000000.0)
            exponent = jnp.exp(scores - jnp.max(scores, axis=-1, keepdims=True))
            prob = to_low(exponent / jnp.sum(exponent, axis=-1, keepdims=True))
            prob_ref[sample, window] = prob
            pieces.append(fold_heads(product(prob, value), mask))
    attended = jnp.concatenate(pieces, axis=0)
    gate = merge_rows(gate_ref[...]).astype(F32)
    gated = to_low(attended * sigmoid(gate))
    gated_ref[...] = gated.reshape(gated_ref.shape)
    cond_proj = merge_rows(cond_proj_ref[...]).astype(F32)
    zero_a, scale_t, shift_t, zero_t = atom_conditions(cond_proj, scale_ref[...], zero_ref[...])
    single = merge_rows(single_ref[...]).astype(F32)
    middle = single + zero_a * product(gated, out_weight_ref[...])
    middle_ref[...] = middle.reshape(middle_ref.shape)
    entering = to_low(norm_rows(middle)[0] * scale_t + shift_t)
    gate_up = to_low(product(entering, up_ref[...])).astype(F32)
    hidden = to_low(jax.nn.silu(gate_up[:, :FFA]) * gate_up[:, FFA:])
    final = middle + zero_t * product(hidden, down_ref[...])
    member = member_rows(token_ref, tokens)
    member_low = member.astype(F32).astype(BF16)
    counts_ref[...] += jnp.broadcast_to(
        jnp.sum(member.astype(F32), axis=1, keepdims=True), counts_ref.shape
    )
    high, rest = split_low(final)
    for sample in range(samples):
        part = slice(sample * ROWS_Q, (sample + 1) * ROWS_Q)
        pooled_ref[sample] += product(member_low, high[part]) + product(member_low, rest[part])

    @pl.when(step == pl.num_programs(0) - 1)
    def _():
        for sample in range(samples):
            pooled_ref[sample] = pooled_ref[sample] / counts_ref[...]


def atom_second(
    atoms_all, starts, query, gate, cond_proj, single, extended, bias, token_row,
    scale_bias, zero_bias, out_weight, up_weight, down_weight, tokens,
):
    samples, atoms, _ = query.shape

    def rows(width):
        return pl.BlockSpec((samples, ROWS_Q, width), lambda i, s: (0, i, 0))

    def kernel(*refs):
        atom_second_kernel(atoms_all, *refs)

    return pl.pallas_call(
        kernel,
        grid_spec=pltpu.PrefetchScalarGridSpec(
            num_scalar_prefetch=1,
            grid=(atoms // ROWS_Q,),
            in_specs=[
                rows(DA), rows(DA), rows(6 * DA), rows(DA), whole(extended.shape),
                pl.BlockSpec((CW, HA * WQ, WK), lambda i, s: (i, 0, 0)),
                pl.BlockSpec((1, ROWS_Q), lambda i, s: (0, i)),
                whole(scale_bias.shape), whole(zero_bias.shape), whole(out_weight.shape),
                whole(up_weight.shape), whole(down_weight.shape),
            ],
            out_specs=[
                pl.BlockSpec((samples, CW, HA * WQ, WK), lambda i, s: (0, i, 0, 0)),
                rows(DA), rows(DA), whole((samples, tokens, DA)), whole((tokens, DA)),
            ],
            scratch_shapes=[pltpu.VMEM(wide_shape(extended), F32)],
        ),
        out_shape=[
            struct((samples, atoms // WQ, HA * WQ, WK), BF16),
            struct((samples, atoms, DA), BF16),
            struct((samples, atoms, DA), F32),
            struct((samples, tokens, DA), F32),
            struct((tokens, DA), F32),
        ],
        compiler_params=params(),
        name="atom_second",
    )(
        starts, query, gate, cond_proj, single, extended, bias, token_row, scale_bias, zero_bias,
        out_weight, up_weight, down_weight,
    )


def atom_third_kernel(
    starts_ref, query_ref, gate_ref, cond_proj_ref, extended_ref, prob_ref, gated_ref, middle_ref,
    pooled_ref, token_ref, scale_ref, zero_ref, out_weight_ref, up_ref, down_ref,
    grad_middle_ref, grad_query_ref, grad_gate_ref, grad_ext_ref, grad_bias_ref, grad_cond_ref,
    grad_out_ref, grad_up_ref, grad_down_ref, sums_ref, wide_ref,
):
    step = pl.program_id(0)
    samples = query_ref.shape[0]
    tokens = pooled_ref.shape[1]

    @pl.when(step == 0)
    def _():
        wide_ref[:, : extended_ref.shape[1], :] = extended_ref[...].astype(F32)
        grad_ext_ref[...] = jnp.zeros_like(grad_ext_ref)
        grad_out_ref[...] = jnp.zeros_like(grad_out_ref)
        grad_up_ref[...] = jnp.zeros_like(grad_up_ref)
        grad_down_ref[...] = jnp.zeros_like(grad_down_ref)
        sums_ref[...] = jnp.zeros_like(sums_ref)

    member = member_rows(token_ref, tokens).astype(F32).astype(BF16)
    grads = []
    for sample in range(samples):
        high, rest = split_low(pooled_ref[sample])
        grads.append(product_left(member, high) + product_left(member, rest))
    grad_stream = jnp.concatenate(grads, axis=0)

    cond_proj = merge_rows(cond_proj_ref[...]).astype(F32)
    zero_a, scale_t, shift_t, zero_t = atom_conditions(cond_proj, scale_ref[...], zero_ref[...])
    normed, inverse = norm_rows(merge_rows(middle_ref[...]))
    entering = to_low(normed * scale_t + shift_t)
    gate_up = to_low(product(entering, up_ref[...])).astype(F32)
    gate_part = gate_up[:, :FFA]
    up_part = gate_up[:, FFA:]
    sig = sigmoid(gate_part)
    silu = gate_part * sig
    hidden = to_low(silu * up_part)
    branch = product(hidden, down_ref[...])
    grad_branch = to_low(grad_stream * zero_t)
    grad_zero_t = grad_stream * branch * zero_t * (1.0 - zero_t)
    grad_down_ref[...] += product_left(hidden, grad_branch)
    grad_hidden = product_right(grad_branch, down_ref[...])
    grad_gate_up = to_low(
        jnp.concatenate(
            [
                grad_hidden * up_part * (sig * (1.0 + gate_part * (1.0 - sig))),
                grad_hidden * silu,
            ],
            axis=1,
        )
    )
    grad_up_ref[...] += product_left(entering, grad_gate_up)
    grad_entering = product_right(grad_gate_up, up_ref[...])
    grad_scale_t = grad_entering * normed * scale_t * (1.0 - scale_t)
    grad_middle = grad_stream + norm_back(grad_entering * scale_t, normed, inverse)
    grad_middle_ref[...] = grad_middle.reshape(grad_middle_ref.shape)

    gated = merge_rows(gated_ref[...])
    branch_a = product(gated, out_weight_ref[...])
    grad_zero_a = grad_middle * branch_a * zero_a * (1.0 - zero_a)
    grad_branch_a = to_low(grad_middle * zero_a)
    grad_out_ref[...] += product_left(gated, grad_branch_a)
    grad_gated = product_right(grad_branch_a, out_weight_ref[...])
    gate_sig = sigmoid(merge_rows(gate_ref[...]).astype(F32))
    grad_gate = grad_gated * gated.astype(F32) * (1.0 - gate_sig)
    grad_gate_ref[...] = to_low(grad_gate).reshape(grad_gate_ref.shape)
    grad_attended = to_low(grad_gated * gate_sig)

    grad_cond_ref[...] = to_low(
        jnp.concatenate([grad_zero_a, grad_scale_t, grad_entering, grad_zero_t], axis=1)
    ).reshape(grad_cond_ref.shape)
    sums_ref[:, :DA] += eight_sums(grad_zero_a)
    sums_ref[:, DA : 2 * DA] += eight_sums(grad_scale_t)
    sums_ref[:, 2 * DA :] += eight_sums(grad_zero_t)

    mask = head_masks()
    grad_bias = [None] * CW
    for sample in range(samples):
        for window in range(CW):
            start = starts_ref[0, step * CW + window]
            first = sample * ROWS_Q + window * WQ
            keyval = window_load(wide_ref, sample, start)
            key = to_low(keyval[:, :DA])
            value = to_low(keyval[:, DA:])
            query = stack_heads(query_ref[sample, window * WQ : (window + 1) * WQ, :], mask)
            grad_wide = stack_heads(grad_attended[first : first + WQ], mask)
            prob = prob_ref[sample, window]
            prob_wide = prob.astype(F32)
            grad_prob = product_right(grad_wide, value)
            inner = jnp.sum(prob_wide * grad_prob, axis=-1, keepdims=True)
            grad_scores = to_low(prob_wide * (grad_prob - inner))
            wide = grad_scores.astype(F32)
            grad_bias[window] = wide if sample == 0 else grad_bias[window] + wide
            grad_query = fold_heads(product(grad_scores, key), mask) * DHA ** (-0.5)
            grad_query_ref[sample, window * WQ : (window + 1) * WQ, :] = to_low(grad_query)
            grad_key = product_left(grad_scores, query) * DHA ** (-0.5)
            grad_value = product_left(prob, grad_wide)
            window_add(
                grad_ext_ref, sample, start, jnp.concatenate([grad_key, grad_value], axis=1)
            )
    for window in range(CW):
        grad_bias_ref[window] = to_low(grad_bias[window])


def atom_third(
    starts, query, gate, cond_proj, extended, prob, gated, middle, grad_pooled, token_row,
    scale_bias, zero_bias, out_weight, up_weight, down_weight,
):
    samples, atoms, _ = query.shape

    def rows(width):
        return pl.BlockSpec((samples, ROWS_Q, width), lambda i, s: (0, i, 0))

    windows = pl.BlockSpec((CW, HA * WQ, WK), lambda i, s: (i, 0, 0))
    return pl.pallas_call(
        atom_third_kernel,
        grid_spec=pltpu.PrefetchScalarGridSpec(
            num_scalar_prefetch=1,
            grid=(atoms // ROWS_Q,),
            in_specs=[
                rows(DA), rows(DA), rows(6 * DA), whole(extended.shape),
                pl.BlockSpec((samples, CW, HA * WQ, WK), lambda i, s: (0, i, 0, 0)),
                rows(DA), rows(DA), whole(grad_pooled.shape),
                pl.BlockSpec((1, ROWS_Q), lambda i, s: (0, i)),
                whole(scale_bias.shape), whole(zero_bias.shape), whole(out_weight.shape),
                whole(up_weight.shape), whole(down_weight.shape),
            ],
            out_specs=[
                rows(DA), rows(DA), rows(DA), whole(wide_shape(extended)), windows, rows(4 * DA),
                whole(out_weight.shape), whole(up_weight.shape), whole(down_weight.shape),
                whole((8, 3 * DA)),
            ],
            scratch_shapes=[pltpu.VMEM(wide_shape(extended), F32)],
        ),
        out_shape=[
            struct((samples, atoms, DA), F32),
            struct((samples, atoms, DA), BF16),
            struct((samples, atoms, DA), BF16),
            struct(wide_shape(extended), F32),
            struct((atoms // WQ, HA * WQ, WK), BF16),
            struct((samples, atoms, 4 * DA), BF16),
            struct(out_weight.shape, F32),
            struct(up_weight.shape, F32),
            struct(down_weight.shape, F32),
            struct((8, 3 * DA), F32),
        ],
        compiler_params=params(),
        name="atom_third",
    )(
        starts, query, gate, cond_proj, extended, prob, gated, middle, grad_pooled, token_row,
        scale_bias, zero_bias, out_weight, up_weight, down_weight,
    )


def atom_fourth_kernel(
    grad_query_ref, grad_gate_ref, grad_ext_ref, low_ref, high_ref, grad_middle_ref,
    grad_cond_ref, single_ref, cond_ref, cond_proj_ref, scale_ref, proj_weight_ref,
    cond_weight_ref, grad_atoms_ref, grad_conds_ref, grad_proj_ref, grad_cond_weight_ref, sums_ref,
):
    step = pl.program_id(0)
    last = pl.num_programs(0) - 1
    samples, rows, _ = single_ref.shape

    @pl.when(step == 0)
    def _():
        grad_proj_ref[...] = jnp.zeros_like(grad_proj_ref)
        grad_cond_weight_ref[...] = jnp.zeros_like(grad_cond_weight_ref)
        sums_ref[...] = jnp.zeros_like(sums_ref)

    first = (step == 0).astype(F32)
    final = (step == last).astype(F32)
    blank = jnp.zeros((rows - MARGIN, 2 * DA), F32)
    keyvals = []
    for sample in range(samples):
        own = grad_ext_ref[sample, pl.ds(pl.multiple_of(MARGIN + step * rows, 8), rows), :]
        from_low = jnp.concatenate([low_ref[sample].astype(F32) * first, blank], axis=0)
        from_high = jnp.concatenate([blank, high_ref[sample].astype(F32) * final], axis=0)
        keyvals.append(to_low(own + from_low + from_high))
    grad_projected = jnp.concatenate(
        [
            merge_rows(grad_query_ref[...]),
            jnp.concatenate(keyvals, axis=0),
            merge_rows(grad_gate_ref[...]),
        ],
        axis=1,
    )
    cond_proj = merge_rows(cond_proj_ref[...]).astype(F32)
    single = merge_rows(single_ref[...]).astype(F32)
    normed, inverse, scale, entering = atom_entry(single, cond_proj, scale_ref[...])
    grad_proj_ref[...] += product_left(entering, grad_projected)
    grad_entering = product_right(grad_projected, proj_weight_ref[...])
    grad_scale = grad_entering * normed * scale * (1.0 - scale)
    sums_ref[...] += eight_sums(grad_scale)
    grad_atoms = merge_rows(grad_middle_ref[...]) + norm_back(
        grad_entering * scale, normed, inverse
    )
    grad_atoms_ref[...] = grad_atoms.reshape(grad_atoms_ref.shape)
    grad_cond_proj = jnp.concatenate(
        [to_low(grad_scale), to_low(grad_entering), merge_rows(grad_cond_ref[...])], axis=1
    )
    cond_norm, cond_inverse = norm_rows(merge_rows(cond_ref[...]).astype(F32))
    grad_cond_weight_ref[...] += product_left(to_low(cond_norm), grad_cond_proj)
    grad_conds = norm_back(
        product_right(grad_cond_proj, cond_weight_ref[...]), cond_norm, cond_inverse
    )
    grad_conds_ref[...] = grad_conds.reshape(grad_conds_ref.shape)


def atom_fourth(
    grad_query, grad_gate, grad_ext, low, high, grad_middle, grad_cond, single, cond, cond_proj,
    scale_bias, proj_weight, cond_weight,
):
    samples, atoms, _ = single.shape
    step = min(256, atoms)

    def rows(width):
        return pl.BlockSpec((samples, step, width), lambda i: (0, i, 0))

    return pl.pallas_call(
        atom_fourth_kernel,
        grid=(atoms // step,),
        in_specs=[
            rows(DA), rows(DA), whole(grad_ext.shape), whole(low.shape), whole(high.shape),
            rows(DA), rows(4 * DA), rows(DA), rows(DA), rows(6 * DA), whole(scale_bias.shape),
            whole(proj_weight.shape), whole(cond_weight.shape),
        ],
        out_specs=[
            rows(DA), rows(DA), whole(proj_weight.shape), whole(cond_weight.shape), whole((8, DA)),
        ],
        out_shape=[
            struct((samples, atoms, DA), F32),
            struct((samples, atoms, DA), F32),
            struct(proj_weight.shape, F32),
            struct(cond_weight.shape, F32),
            struct((8, DA), F32),
        ],
        compiler_params=params(),
        name="atom_fourth",
    )(
        grad_query, grad_gate, grad_ext, low, high, grad_middle, grad_cond, single, cond,
        cond_proj, scale_bias, proj_weight, cond_weight,
    )


def joined_tokens(ref):
    return jnp.concatenate([ref[source, 0] for source in range(ref.shape[0])], axis=1)


def attend_forward_kernel(heads_ref, bias_ref, out_ref, prob_ref):
    joined = joined_tokens(heads_ref)
    query = joined[:DH]
    key = joined[DH : 2 * DH]
    value = joined[2 * DH :]
    bias = bias_ref[...]
    bias = bias.reshape(bias.shape[0] * bias.shape[2], bias.shape[3]).astype(F32)
    scores = product_left(key, query) * DH ** (-0.5) + bias
    exponent = jnp.exp(scores - jnp.max(scores, axis=0, keepdims=True))
    prob = to_low(exponent / jnp.sum(exponent, axis=0, keepdims=True))
    prob_ref[0, 0] = prob
    attended = to_low(product(value, prob))
    tokens = out_ref.shape[3]
    for source in range(out_ref.shape[0]):
        out_ref[source, 0] = attended[:, source * tokens : (source + 1) * tokens]


def attend_forward(heads_view, bias_full):
    groups, samples, width, tokens = heads_view.shape
    parts, heads, keys, rows = bias_full.shape
    return pl.pallas_call(
        attend_forward_kernel,
        grid=(heads, samples),
        in_specs=[
            pl.BlockSpec((groups, 1, 3 * DH, tokens), lambda h, s: (0, s, h, 0)),
            pl.BlockSpec((parts, 1, keys, rows), lambda h, s: (0, h, 0, 0)),
        ],
        out_specs=[
            pl.BlockSpec((groups, 1, DH, tokens), lambda h, s: (0, s, h, 0)),
            pl.BlockSpec((1, 1, rows, rows), lambda h, s: (h, s, 0, 0)),
        ],
        out_shape=[
            struct((groups, samples, heads * DH, tokens), BF16),
            struct((heads, samples, rows, rows), BF16),
        ],
        compiler_params=params(),
        name="attend_forward",
    )(heads_view, bias_full)


def attend_backward_kernel(heads_ref, prob_ref, grad_ref, out_ref, bias_ref, total_ref):
    sample = pl.program_id(1)
    joined = joined_tokens(heads_ref)
    query = joined[:DH]
    key = joined[DH : 2 * DH]
    value = joined[2 * DH :]
    grad = joined_tokens(grad_ref)
    prob = prob_ref[0, 0]
    wide = prob.astype(F32)
    grad_value = product_right(grad, prob)
    grad_prob = product_left(value, grad)
    inner = jnp.sum(wide * grad_prob, axis=0, keepdims=True)
    grad_scores = to_low(wide * (grad_prob - inner))
    grad_query = product(key, grad_scores) * DH ** (-0.5)
    grad_key = product_right(query, grad_scores) * DH ** (-0.5)
    stacked = to_low(jnp.concatenate([grad_query, grad_key, grad_value], axis=0))
    tokens = out_ref.shape[3]
    for source in range(out_ref.shape[0]):
        out_ref[source, 0] = stacked[:, source * tokens : (source + 1) * tokens]

    @pl.when(sample == 0)
    def _():
        total_ref[...] = grad_scores.astype(F32)

    @pl.when(sample > 0)
    def _():
        total_ref[...] += grad_scores.astype(F32)

    @pl.when(sample == pl.num_programs(1) - 1)
    def _():
        bias_ref[...] = to_low(total_ref[...]).reshape(bias_ref.shape)


def attend_backward(heads_view, prob, grad_view, parts):
    groups, samples, width, tokens = heads_view.shape
    heads, _, rows, _ = prob.shape
    keys = rows // parts
    return pl.pallas_call(
        attend_backward_kernel,
        grid=(heads, samples),
        in_specs=[
            pl.BlockSpec((groups, 1, 3 * DH, tokens), lambda h, s: (0, s, h, 0)),
            pl.BlockSpec((1, 1, rows, rows), lambda h, s: (h, s, 0, 0)),
            pl.BlockSpec((groups, 1, DH, tokens), lambda h, s: (0, s, h, 0)),
        ],
        out_specs=[
            pl.BlockSpec((groups, 1, 3 * DH, tokens), lambda h, s: (0, s, h, 0)),
            pl.BlockSpec((parts, 1, keys, rows), lambda h, s: (0, h, 0, 0)),
        ],
        out_shape=[
            struct(heads_view.shape, BF16),
            struct((parts, heads, keys, rows), BF16),
        ],
        scratch_shapes=[pltpu.VMEM((rows, rows), F32)],
        compiler_params=params(),
        name="attend_backward",
    )(heads_view, prob, grad_view)


def conditioning(cond_proj, scale_bias, zero_bias, width):
    return (
        sigmoid(cond_proj[:, :width] + scale_bias[:width]),
        cond_proj[:, width : 2 * width],
        sigmoid(cond_proj[:, 2 * width : 3 * width] + zero_bias[:width]),
        sigmoid(cond_proj[:, 3 * width : 4 * width] + scale_bias[width:]),
        cond_proj[:, 4 * width : 5 * width],
        sigmoid(cond_proj[:, 5 * width :] + zero_bias[width:]),
    )


def transition_forward(stream, scale_gate, shift_part, zero_gate, up_weight, down_weight):
    normed, inverse = norm_rows(stream)
    entering = to_low(normed * scale_gate + shift_part)
    gate_up = to_low(product(entering, up_weight))
    gate_part = gate_up[:, :FF].astype(F32)
    up_part = gate_up[:, FF:].astype(F32)
    hidden = to_low(jax.nn.silu(gate_part) * up_part)
    branch = product(hidden, down_weight)
    return (
        stream + zero_gate * branch,
        (normed, inverse, entering, gate_part, up_part, hidden, branch),
    )


def transition_backward(grad_stream, saved_state, scale_gate, zero_gate, up_weight, down_weight):
    normed, inverse, entering, gate_part, up_part, hidden, branch = saved_state
    grad_branch = to_low(grad_stream * zero_gate)
    grad_zero_pre = grad_stream * branch * zero_gate * (1.0 - zero_gate)
    grad_down = to_low(product_left(hidden, grad_branch))
    grad_hidden = product_right(grad_branch, down_weight)
    sigmoid_gate = sigmoid(gate_part)
    grad_gate = grad_hidden * up_part * (sigmoid_gate * (1.0 + gate_part * (1.0 - sigmoid_gate)))
    grad_up_part = grad_hidden * gate_part * sigmoid_gate
    grad_gate_up = to_low(jnp.concatenate([grad_gate, grad_up_part], axis=1))
    grad_up = to_low(product_left(entering, grad_gate_up))
    grad_entering = product_right(grad_gate_up, up_weight)
    grad_scale_pre = grad_entering * normed * scale_gate * (1.0 - scale_gate)
    grad_input = grad_stream + norm_back(grad_entering * scale_gate, normed, inverse)
    return (grad_input, (grad_scale_pre, grad_entering, grad_zero_pre), grad_up, grad_down)


def direct_exchange():
    return lax.axis_size("dp") == 8 and lax.axis_size("seq") == 4


def bit(axis, mask):
    return (lax.axis_index(axis) // mask) % 2


def xor_send(block, axis, mask):
    count = lax.axis_size(axis)
    return lax.ppermute(block, axis, [(i, i ^ mask) for i in range(count)])


def add_low(left_side, right_side):
    return to_low(left_side.astype(F32) + right_side.astype(F32))


def row_half(block, index):
    rows = block.shape[0] // 2
    return lax.dynamic_slice_in_dim(block, index * rows, rows, 0)


def reduce_rows(block, steps):
    for axis, mask in steps:
        mine = bit(axis, mask)
        received = xor_send(row_half(block, 1 - mine), axis, mask)
        block = add_low(row_half(block, mine), received)
    return block


def gather_rows(block, steps):
    for axis, mask in reversed(steps):
        received = xor_send(block, axis, mask)
        block = jnp.where(
            bit(axis, mask) == 0,
            jnp.concatenate([block, received], axis=0),
            jnp.concatenate([received, block], axis=0),
        )
    return block


def place_columns_kernel(place_ref, *refs):
    pieces, out_ref = refs[:-1], refs[-1]
    width = pieces[0].shape[1]
    for index, piece in enumerate(pieces):
        column = pl.multiple_of((index ^ place_ref[0]) * width, 128)
        out_ref[:, pl.ds(column, width)] = piece[...].astype(F32)


def place_columns(pieces, place):
    rows, width = pieces[0].shape
    step = rows // 4 if rows >= 512 else rows
    return pl.pallas_call(
        place_columns_kernel,
        grid_spec=pltpu.PrefetchScalarGridSpec(
            num_scalar_prefetch=1,
            grid=(rows // step,),
            in_specs=[pl.BlockSpec((step, width), lambda i, p: (i, 0)) for _ in pieces],
            out_specs=pl.BlockSpec((step, width * len(pieces)), lambda i, p: (i, 0)),
        ),
        out_shape=struct((rows, width * len(pieces)), F32),
        compiler_params=params(),
        name="place_columns",
    )(place.reshape(1).astype(jnp.int32), *pieces)


def column_place(first):
    return bit("dp", 1) * 2 + bit("dp", first)


def quarter_products(left_side, right_side, left_dim, right_dim, first):
    width = right_side.shape[right_dim] // 4
    place = column_place(first)
    blocks = []
    for index in range(4):
        part = lax.dynamic_slice_in_dim(
            right_side, (index ^ place) * width, width, right_dim
        )
        blocks.append(to_low(contract(left_side, part, left_dim, 1 - right_dim)))
    return blocks


def quarter_slices(values, first):
    width = values.shape[1] // 4
    place = column_place(first)
    return [
        lax.dynamic_slice_in_dim(values, (index ^ place) * width, width, 1) for index in range(4)
    ]


CORE, FIRST, SECOND, LINE, LINE_BACK, SECOND_BACK, FIRST_BACK, CORE_BACK = 0, 2, 3, 4, 7, 10, 11, 12
COPIES = 14
SLAB = 16


class Chunk:
    def __init__(self, number, blocks, outs, first_row, rows, first, second, scratch, sems):
        self.number, self.rows = number, rows
        self.blocks = [block.at[pl.ds(first_row, rows)] for block in blocks]
        self.outs = [out.at[pl.ds(first_row, rows)] for out in outs]
        self.from_core, self.far, self.near, self.from_first, self.half, self.parts = scratch[:6]
        self.from_second, self.from_line = scratch[6:]
        self.sends, self.receives = sems
        self.width = self.near.shape[1]
        dp, seq = lax.axis_index("dp"), lax.axis_index("seq")
        self.core_id = {"dp": dp ^ 1}
        self.first_id = {"dp": dp ^ first}
        self.second_id = {"dp": dp ^ second}
        self.line_ids = [{"seq": seq ^ mask} for mask in (1, 2, 3)]
        self.seq = seq
        self.mine = (dp // second) % 2

    def copy(self, index, source, target, device):
        return pltpu.make_async_remote_copy(
            src_ref=source,
            dst_ref=target,
            send_sem=self.sends.at[self.number, index],
            recv_sem=self.receives.at[self.number, index],
            device_id=device,
            device_id_type=pl.DeviceIdType.MESH,
        )

    def slabs(self, rows, body):
        def step(index, carry):
            body(pl.multiple_of(index * SLAB, SLAB))
            return carry

        lax.fori_loop(0, rows // SLAB, step, 0)

    def leg_0(self):
        self.core_copies = [
            self.copy(CORE + i, self.blocks[2 + i], self.from_core.at[i], self.core_id)
            for i in (1, 0)
        ]
        for copy in self.core_copies:
            copy.start()

    def leg_1(self):
        self.core_copies[0].wait()

        def add_far(row):
            rows = pl.ds(row, SLAB)
            self.far[rows, :] = add_low(self.blocks[1][rows, :], self.from_core[1, rows, :])

        self.slabs(self.rows, add_far)
        self.first_copy = self.copy(FIRST, self.far, self.from_first, self.first_id)
        self.first_copy.start()
        self.core_copies[1].wait()

        def add_near(row):
            rows = pl.ds(row, SLAB)
            self.near[rows, :] = add_low(self.blocks[0][rows, :], self.from_core[0, rows, :])

        self.slabs(self.rows, add_near)

    def leg_2(self):
        self.first_copy.wait()
        half = self.rows // 2

        def add_theirs(row):
            rows = pl.ds(pl.multiple_of((1 - self.mine) * half + row, SLAB), SLAB)
            self.half[pl.ds(row, SLAB), :] = add_low(self.near[rows, :], self.from_first[rows, :])

        self.slabs(half, add_theirs)
        self.second_copy = self.copy(SECOND, self.half, self.from_second, self.second_id)
        self.second_copy.start()

        def add_mine(row):
            rows = pl.ds(pl.multiple_of(self.mine * half + row, SLAB), SLAB)
            self.near[rows, :] = add_low(self.near[rows, :], self.from_first[rows, :])

        self.slabs(half, add_mine)

    def leg_3(self):
        self.second_copy.wait()
        half = self.rows // 2

        def add(row):
            rows = pl.ds(pl.multiple_of(self.mine * half + row, SLAB), SLAB)
            self.parts[pl.ds(row, SLAB), :] = add_low(
                self.near[rows, :], self.from_second[pl.ds(row, SLAB), :]
            )

        self.slabs(half, add)
        part = half // 4
        self.line_copies = []
        for index, mask in enumerate((1, 2, 3)):
            source = pl.multiple_of((self.seq ^ mask) * part, SLAB)
            self.line_copies.append(
                self.copy(
                    LINE + index,
                    self.parts.at[pl.ds(source, part)],
                    self.from_line.at[index],
                    self.line_ids[index],
                )
            )
        for copy in self.line_copies:
            copy.start()

    def leg_4(self):
        for copy in self.line_copies:
            copy.wait()
        half = self.rows // 2
        part = half // 4

        def add(row):
            rows = pl.ds(pl.multiple_of(self.seq * part + row, SLAB), SLAB)
            local = pl.ds(row, SLAB)
            total = self.parts[rows, :].astype(F32)
            for index in range(3):
                total = total + self.from_line[index, local, :].astype(F32)
            target = pl.multiple_of(self.mine * half + self.seq * part + row, SLAB)
            self.outs[0][pl.ds(target, SLAB), :] = to_low(total)

        self.slabs(part, add)
        place = pl.ds(pl.multiple_of(self.mine * half + self.seq * part, SLAB), part)
        mine = self.outs[0].at[place]
        self.line_backs = [
            self.copy(LINE_BACK + index, mine, mine, self.line_ids[index]) for index in range(3)
        ]
        for copy in self.line_backs:
            copy.start()

    def leg_5(self):
        for copy in self.line_backs:
            copy.wait()
        half = self.rows // 2
        mine = self.outs[0].at[pl.ds(pl.multiple_of(self.mine * half, SLAB), half)]
        self.second_back = self.copy(SECOND_BACK, mine, mine, self.second_id)
        self.second_back.start()

    def leg_6(self):
        self.second_back.wait()
        self.first_back = self.copy(FIRST_BACK, self.outs[0], self.outs[1], self.first_id)
        self.first_back.start()
        self.core_back = self.copy(CORE_BACK, self.outs[0], self.outs[2], self.core_id)
        self.core_back.start()

    def leg_7(self):
        self.first_back.wait()
        self.last_back = self.copy(CORE_BACK + 1, self.outs[1], self.outs[3], self.core_id)
        self.last_back.start()

    def leg_8(self):
        self.core_back.wait()
        self.last_back.wait()


def sum_quarters_kernel(plan, arrays, *refs):
    count = len(arrays)
    inputs, outs = refs[: 4 * count], refs[4 * count : 8 * count]
    scratch, sems = refs[8 * count : -2], refs[-2:]
    chunks = []
    for number, (array, first_row, rows, first, second, lag) in enumerate(plan):
        chunks.append(
            (
                lag,
                Chunk(
                    number,
                    inputs[4 * array : 4 * array + 4],
                    outs[4 * array : 4 * array + 4],
                    first_row,
                    rows,
                    first,
                    second,
                    scratch[8 * number : 8 * number + 8],
                    sems,
                ),
            )
        )
    legs = sorted(
        ((leg + lag, number, leg) for leg in range(9) for number, (lag, _) in enumerate(chunks)),
    )
    for _, number, leg in legs:
        getattr(chunks[number][1], f"leg_{leg}")()


def sum_quarters(arrays, plan):
    blocks = [block for array in arrays for block in array]
    scratch = []
    for array, _, rows, _, _, _ in plan:
        width = arrays[array][0].shape[1]
        scratch += [
            pltpu.VMEM((2, rows, width), BF16),
            pltpu.VMEM((rows, width), BF16),
            pltpu.VMEM((rows, width), BF16),
            pltpu.VMEM((rows, width), BF16),
            pltpu.VMEM((rows // 2, width), BF16),
            pltpu.VMEM((rows // 2, width), BF16),
            pltpu.VMEM((rows // 2, width), BF16),
            pltpu.VMEM((3, rows // 8, width), BF16),
        ]
    sems = [pltpu.SemaphoreType.DMA((len(plan), COPIES)) for _ in range(2)]

    def kernel(*refs):
        sum_quarters_kernel(plan, arrays, *refs)

    outs = pl.pallas_call(
        kernel,
        in_specs=[pl.BlockSpec(memory_space=pltpu.VMEM) for _ in blocks],
        out_specs=[pl.BlockSpec(memory_space=pltpu.VMEM) for _ in blocks],
        out_shape=[struct(block.shape, BF16) for block in blocks],
        scratch_shapes=scratch + sems,
        compiler_params=params(has_side_effects=True),
        name="sum_quarters",
    )(*blocks)
    return [outs[4 * index : 4 * index + 4] for index in range(len(arrays))]


def summed_late(proj_sides, cond_sides, late):
    if not direct_exchange():
        local = (
            contract(proj_sides[0], proj_sides[1], 0, 1),
            contract(cond_sides[0], cond_sides[1], 0, 0),
            late,
        )
        sums = lax.psum(tuple(to_low(value) for value in local), ("dp", "seq"))
        return tuple(value.astype(F32) for value in sums)
    proj = quarter_products(proj_sides[0], proj_sides[1], 0, 0, 2)
    cond = quarter_products(cond_sides[0], cond_sides[1], 0, 1, 4)
    rest = quarter_slices(to_low(late), 2)
    rows = proj[0].shape[0] // 2
    plan = (
        (0, 0, rows, 2, 4, 0.0),
        (1, 0, cond[0].shape[0], 4, 2, 0.4),
        (0, rows, rows, 2, 4, 1.0),
        (2, 0, rest[0].shape[0], 2, 4, 1.2),
    )
    sums = sum_quarters((proj, cond, rest), plan)
    return tuple(
        place_columns(pieces, column_place(first)) for pieces, first in zip(sums, (2, 4, 2))
    )


def summed_rows(values):
    if not direct_exchange():
        return lax.psum(values, "dp")
    steps = (("dp", 1), ("dp", 2), ("dp", 4))
    return gather_rows(reduce_rows(values, steps), steps)


def scattered_rows(values):
    if not direct_exchange():
        return lax.psum_scatter(values, "dp", scatter_dimension=0, tiled=False)
    steps = (("dp", 4), ("dp", 2), ("dp", 1))
    return reduce_rows(values, steps)[0]


PIECE = 384


def place_weights_kernel(shapes, place_ref, *refs):
    count = len(shapes)
    stacks, shards, outs = refs[:8], refs[8 : 8 + count], refs[8 + count :]
    relative = pl.program_id(0) ^ place_ref[1]

    @pl.when(relative == 0)
    def _():
        for shard, out in zip(shards, outs):
            out[...] = shard[...]

    @pl.when(relative != 0)
    def _():
        for index, stack in enumerate(stacks):
            owner = index ^ place_ref[0]
            first = 0
            for (row_parts, rows, width), out in zip(shapes, outs):
                row = pl.multiple_of((owner % row_parts) * rows, 16)
                column = (owner // row_parts) * width
                for offset in range(0, width, PIECE):
                    out[pl.ds(row, rows), pl.ds(pl.multiple_of(column + offset, 128), PIECE)] = (
                        stack[0, first : first + rows, :]
                    )
                    first += rows


def gather_line(shards, column_parts, after=None):
    if not direct_exchange():
        return None
    place = lax.axis_index("dp")
    shapes, slabs = [], []
    for shard, columns in zip(shards, column_parts):
        row_parts = 8 // columns
        rows, width = shard.shape[0] // row_parts, shard.shape[1] // columns
        shapes.append((row_parts, rows, width))
        piece = lax.dynamic_slice(
            shard, ((place % row_parts) * rows, (place // row_parts) * width), (rows, width)
        )
        slabs += [piece[:, offset : offset + PIECE] for offset in range(0, width, PIECE)]
    slab = jnp.concatenate(slabs, axis=0)
    if after is not None:
        slab, _ = lax.optimization_barrier((slab, after))
    stack = jnp.stack([xor_send(slab, "seq", mask) for mask in (1, 2, 3)])
    return shapes, stack


def gather_plane(stack):
    return [stack] + [xor_send(stack, "dp", mask) for mask in (2, 4, 6)]


def gather_weights(shards, shapes, even):
    groups = lax.axis_size("seq")
    if not direct_exchange():
        return tuple(lax.all_gather(shard, "seq", axis=0, tiled=True) for shard in shards)
    stacks = []
    for item in even:
        stacks += [item, xor_send(item, "dp", 1)]
    block = (1,) + even[0].shape[1:]

    def kernel(*refs):
        place_weights_kernel(shapes, *refs)

    return pl.pallas_call(
        kernel,
        grid_spec=pltpu.PrefetchScalarGridSpec(
            num_scalar_prefetch=1,
            grid=(groups,),
            in_specs=[
                pl.BlockSpec(block, lambda i, p: (jnp.maximum((i ^ p[1]) - 1, 0), 0, 0))
                for _ in stacks
            ]
            + [whole(shard.shape) for shard in shards],
            out_specs=[pl.BlockSpec(shard.shape, lambda i, p: (i, 0)) for shard in shards],
        ),
        out_shape=[
            struct((groups * shard.shape[0], shard.shape[1]), shard.dtype) for shard in shards
        ],
        compiler_params=params(),
        name="place_weights",
    )(
        jnp.stack([lax.axis_index("dp"), lax.axis_index("seq")]).astype(jnp.int32),
        *stacks, *shards,
    )


def swap(block):
    return lax.all_to_all(block, "seq", split_axis=0, concat_axis=0, tiled=True)


def neighbour_rows(to_next, to_previous):
    count = lax.axis_size("seq")
    forward = [(i, i + 1) for i in range(count - 1)]
    backward = [(i + 1, i) for i in range(count - 1)]
    return (
        lax.ppermute(to_next, "seq", forward),
        lax.ppermute(to_previous, "seq", backward),
    )


def per_device(
    atom_single,
    atom_cond,
    token_single,
    token_cond,
    atom_pair,
    token_pair,
    atom_token,
    window_shift,
    noise_bin,
    out_cotangent,
    atom_cond_weight,
    atom_scale_bias,
    atom_zero_bias,
    atom_projection,
    atom_output,
    atom_pair_weight,
    atom_up_weight,
    atom_down_weight,
    pool_weight,
    cond_weight,
    scale_bias,
    zero_bias,
    token_projection,
    token_output,
    token_pair_weight,
    token_up_weight,
    token_down_weight,
):
    groups = lax.axis_size("seq")
    parts = lax.axis_size("dp")
    place = lax.axis_index("seq")
    samples, atoms_dev, _ = atom_single.shape
    tokens_dev = token_single.shape[1]
    rows_token = samples * tokens_dev
    windows_dev = atoms_dev // WQ
    heads_dev = H // groups
    keys_dev = token_pair.shape[1]
    tokens_all = tokens_dev * groups

    first_shards = (cond_weight, token_projection)
    second_shards = (token_output, token_up_weight, token_down_weight)
    shapes_first = shapes_second = even_first = even_second = None
    if direct_exchange():
        shapes_first, stack_first = gather_line(first_shards, (4, 4))
        shapes_second, stack_second = gather_line(second_shards, (2, 4, 2), stack_first)
        even_first = gather_plane(stack_first)

    pair_norm_token, pair_inverse_token = norm_rows(token_pair.astype(F32))
    pair_low = to_low(pair_norm_token)
    bias_local = to_low(
        jnp.einsum("rkc,ch->hkr", pair_low, token_pair_weight, preferred_element_type=F32)
    )
    bias_swapped = swap(bias_local.reshape(groups, heads_dev, keys_dev, tokens_dev))
    bias_heads = bias_swapped.transpose(1, 2, 0, 3).reshape(heads_dev, keys_dev, tokens_all)
    bias_full = lax.all_gather(bias_heads, "dp", axis=0, tiled=False)

    key_lane = jnp.arange(LANES) // CP
    spread = to_low((key_lane[:, None] == key_lane[None, :]).astype(F32) / CP)
    pair_key = jnp.arange(WK * CP) // CP
    expand = to_low(jnp.arange(WK)[:, None] == pair_key[None, :])
    pair_wide = (
        jnp.eye(WK, dtype=BF16)[:, None, None, :] * atom_pair_weight[None, :, :, None]
    ).reshape(WK * CP, HA * WK)
    pair_weight_rows = jnp.tile(atom_pair_weight.astype(F32).T, (1, WK))
    pair_rows = atom_pair.reshape(windows_dev * WQ, WK * CP)
    bias_atom = pair_forward(pair_rows, spread, pair_wide)

    atom_scale = atom_scale_bias.astype(F32).reshape(1, 2 * DA)
    atom_zero = atom_zero_bias.astype(F32).reshape(1, 2 * DA)
    query_atom, keyval_atom, gate_atom, cond_proj_atom = atom_first(
        atom_single, atom_cond, atom_cond_weight, atom_scale, atom_projection
    )
    from_low, from_high = neighbour_rows(
        keyval_atom[:, atoms_dev - MARGIN :], keyval_atom[:, :MARGIN]
    )
    extended = jnp.concatenate([from_low, keyval_atom, from_high], axis=1)
    first_key = jnp.arange(windows_dev, dtype=jnp.int32) * WQ - (WK - WQ) // 2 + window_shift
    starts = jnp.stack([first_key + MARGIN, first_key + place * atoms_dev])
    token_row = (atom_token - place * tokens_dev).reshape(1, atoms_dev)
    if direct_exchange():
        stack_second, bias_atom = lax.optimization_barrier((stack_second, bias_atom))
        even_second = gather_plane(stack_second)
    prob_atom, gated_atom, middle_atom, pooled, counts = atom_second(
        atoms_dev * groups, starts, query_atom, gate_atom, cond_proj_atom, atom_single, extended,
        bias_atom, token_row, atom_scale, atom_zero, atom_output, atom_up_weight,
        atom_down_weight, tokens_dev,
    )

    cond_full, projection_full = gather_weights(first_shards, shapes_first, even_first)
    pooled_low = to_low(pooled).reshape(rows_token, DA)
    token_start = token_single.astype(F32).reshape(rows_token, D) + product(
        pooled_low, pool_weight
    )
    cond_norm, cond_inverse = norm_rows(token_cond.astype(F32).reshape(rows_token, CS))
    cond_low = to_low(cond_norm)
    cond_proj = to_low(product(cond_low, cond_full)).astype(F32)
    scale_a_tok, shift_a_tok, zero_a_tok, scale_t_tok, shift_t_tok, zero_t_tok = conditioning(
        cond_proj, scale_bias.astype(F32), zero_bias.astype(F32), D
    )
    if direct_exchange():
        token_start, *even_second = lax.optimization_barrier((token_start, *even_second))
    output_full, up_full, down_full = gather_weights(second_shards, shapes_second, even_second)
    normed_token, inverse_token = norm_rows(token_start)
    entering_token = to_low(normed_token * scale_a_tok + shift_a_tok)
    projected = to_low(contract(projection_full, entering_token, 0, 1)).reshape(
        groups, heads_dev, 4 * DH, samples, tokens_dev
    )
    heads_view = swap(
        projected[:, :, : 3 * DH]
        .transpose(0, 3, 1, 2, 4)
        .reshape(groups, samples, heads_dev * 3 * DH, tokens_dev)
    )
    gate_sig_token = sigmoid(projected[:, :, 3 * DH :].reshape(D, rows_token).astype(F32))
    attended_swapped, prob_token = attend_forward(heads_view, bias_full)
    attended_token = (
        swap(attended_swapped).transpose(0, 2, 1, 3).reshape(D, rows_token).astype(F32)
    )
    gated_token = to_low(attended_token * gate_sig_token)
    branch_token = product_left(gated_token, output_full)
    middle_token = token_start + zero_a_tok * branch_token
    final_token, saved_token = transition_forward(
        middle_token, scale_t_tok, shift_t_tok, zero_t_tok, up_full, down_full
    )
    block_out = final_token.astype(BF16).reshape(samples, tokens_dev, D)

    loss_weight = noise_weight(noise_bin)
    grad_final = (out_cotangent.astype(F32) * loss_weight[:, None, None]).reshape(rows_token, D)
    grad_middle_token, trans_grads_tok, grad_token_up, grad_token_down = transition_backward(
        grad_final, saved_token, scale_t_tok, zero_t_tok, up_full, down_full
    )
    grad_branch_token = to_low(grad_middle_token * zero_a_tok)
    grad_zero_pre = grad_middle_token * branch_token * zero_a_tok * (1.0 - zero_a_tok)
    grad_token_out = to_low(product(gated_token, grad_branch_token))
    grad_gated = to_low(product_right(output_full, grad_branch_token)).astype(F32)
    grad_attended = to_low(grad_gated * gate_sig_token)
    grad_attended, *early = lax.optimization_barrier(
        (grad_attended, grad_token_up, grad_token_down, grad_token_out)
    )
    with jax.named_scope("early_sum"):
        early = lax.psum(tuple(early), ("dp", "seq"))
    grad_gate_token = to_low(
        grad_gated * attended_token * gate_sig_token * (1.0 - gate_sig_token)
    )
    grad_view = swap(
        grad_attended.reshape(groups, heads_dev * DH, samples, tokens_dev).transpose(0, 2, 1, 3)
    )
    grad_heads, grad_bias = attend_backward(heads_view, prob_token, grad_view, parts)
    grad_rows = (
        swap(grad_heads)
        .transpose(0, 2, 1, 3)
        .reshape(groups, heads_dev, 3 * DH, rows_token)
    )
    grad_projected = jnp.concatenate(
        [grad_rows, grad_gate_token.reshape(groups, heads_dev, DH, rows_token)], axis=2
    ).reshape(4 * D, rows_token)
    grad_entering_token = contract(grad_projected, projection_full, 0, 1)
    grad_scale_pre = grad_entering_token * normed_token * scale_a_tok * (1.0 - scale_a_tok)
    grad_cond_proj = to_low(
        jnp.concatenate(
            [
                grad_scale_pre,
                grad_entering_token,
                grad_zero_pre,
                trans_grads_tok[0],
                trans_grads_tok[1],
                trans_grads_tok[2],
            ],
            axis=1,
        )
    )
    grad_cond = norm_back(product_right(grad_cond_proj, cond_full), cond_norm, cond_inverse)
    grad_start = grad_middle_token + norm_back(
        grad_entering_token * scale_a_tok, normed_token, inverse_token
    )
    grad_scale_bias = jnp.concatenate(
        [jnp.sum(grad_scale_pre, axis=0), jnp.sum(trans_grads_tok[0], axis=0)]
    )
    grad_zero_bias = jnp.concatenate(
        [jnp.sum(grad_zero_pre, axis=0), jnp.sum(trans_grads_tok[2], axis=0)]
    )
    grad_pool_branch = to_low(grad_start)
    grad_pool = product_left(pooled_low, grad_pool_branch)
    grad_pooled = (
        product_right(grad_pool_branch, pool_weight).reshape(samples, tokens_dev, DA) / counts
    )

    grad_bias_keys = scattered_rows(grad_bias)
    grad_bias_rows = (
        swap(
            grad_bias_keys.reshape(heads_dev, keys_dev, groups, tokens_dev).transpose(2, 0, 1, 3)
        )
        .reshape(H, keys_dev, tokens_dev)
    )
    grad_pair_weight_token = jnp.einsum(
        "rkc,hkr->ch", pair_low, grad_bias_rows, preferred_element_type=F32
    )
    grad_pair_low = jnp.einsum(
        "hkr,ch->rkc", grad_bias_rows, token_pair_weight, preferred_element_type=F32
    )
    grad_token_pair = norm_back(grad_pair_low, pair_norm_token, pair_inverse_token)

    (
        grad_middle_atom, grad_query, grad_gate, grad_ext, grad_bias_atom, grad_cond_atom,
        grad_atom_out, grad_atom_up, grad_atom_down, sums_third,
    ) = atom_third(
        starts, query_atom, gate_atom, cond_proj_atom, extended, prob_atom, gated_atom,
        middle_atom, grad_pooled, token_row, atom_scale, atom_zero, atom_output, atom_up_weight,
        atom_down_weight,
    )
    grad_bias_whole = summed_rows(grad_bias_atom)
    back_low, back_high = neighbour_rows(
        to_low(grad_ext[:, atoms_dev + MARGIN : atoms_dev + 2 * MARGIN]), to_low(grad_ext[:, :MARGIN])
    )
    grad_atoms, grad_atom_conds, grad_atom_proj, grad_atom_cond_weight, sums_fourth = atom_fourth(
        grad_query, grad_gate, grad_ext, back_low, back_high, grad_middle_atom, grad_cond_atom,
        atom_single, atom_cond, cond_proj_atom, atom_scale, atom_projection, atom_cond_weight,
    )
    grad_atom_pair, pair_sums = pair_backward(
        pair_rows, grad_bias_whole, spread, expand, pair_weight_rows
    )
    grad_pair_weight_atom = (
        pair_sums.reshape(HA, 8, WK, CP).sum(axis=(1, 2)).T.reshape(CP * HA) / parts
    )
    sums_third = jnp.sum(sums_third, axis=0)
    grad_atom_scale_bias = jnp.concatenate(
        [jnp.sum(sums_fourth, axis=0), sums_third[DA : 2 * DA]]
    )
    grad_atom_zero_bias = jnp.concatenate([sums_third[:DA], sums_third[2 * DA :]])
    small = jnp.concatenate(
        [
            grad_scale_bias,
            grad_zero_bias,
            grad_atom_scale_bias,
            grad_atom_zero_bias,
            grad_pair_weight_token.reshape(-1),
            grad_pair_weight_atom,
        ]
    )
    small = jnp.pad(small, (0, DA * DA - small.shape[0])).reshape(DA, DA)
    parts_late = (
        grad_pool, grad_atom_cond_weight, grad_atom_proj, grad_atom_out, grad_atom_up,
        grad_atom_down[:DA], grad_atom_down[DA:], small,
    )
    grad_token_proj, grad_cond_full, late_sum = summed_late(
        (entering_token, grad_projected),
        (cond_low, grad_cond_proj),
        jnp.concatenate(parts_late, axis=1),
    )
    late = []
    first = 0
    for part in parts_late:
        late.append(late_sum[:, first : first + part.shape[1]])
        first += part.shape[1]
    small = late[7].reshape(-1)
    pieces = []
    first = 0
    for shape in ((2 * D,), (2 * D,), (2 * DA,), (2 * DA,), (128, H), (CP, HA)):
        size = math.prod(shape)
        pieces.append(small[first : first + size].reshape(shape))
        first += size
    return (
        block_out,
        grad_atoms,
        grad_atom_conds,
        grad_start.reshape(samples, tokens_dev, D),
        grad_cond.reshape(samples, tokens_dev, CS),
        grad_atom_pair.reshape(windows_dev, WQ, WK * CP),
        grad_token_pair,
        late[1],
        pieces[2],
        pieces[3],
        late[2],
        late[3],
        pieces[5],
        late[4],
        jnp.concatenate([late[5], late[6]], axis=0),
        late[0],
        grad_cond_full,
        pieces[0],
        pieces[1],
        grad_token_proj,
        early[2].astype(F32),
        pieces[4],
        early[0].astype(F32),
        early[1].astype(F32),
    )


def solution(mesh):
    in_specs = (
        P("dp", "seq", None),
        P("dp", "seq", None),
        P("dp", "seq", None),
        P("dp", "seq", None),
        P("seq", None, None),
        P("seq", "dp", None),
        P("seq"),
        P("seq"),
        P("dp"),
        P("dp", "seq", None),
        P(),
        P(),
        P(),
        P(),
        P(),
        P(),
        P(),
        P(),
        P(),
        P("seq", None),
        P(),
        P(),
        P("seq", None),
        P("seq", None),
        P(),
        P("seq", None),
        P("seq", None),
    )
    out_specs = (
        P("dp", "seq", None),
        P("dp", "seq", None),
        P("dp", "seq", None),
        P("dp", "seq", None),
        P("dp", "seq", None),
        P("seq", None, None),
        P("seq", "dp", None),
    ) + (P(),) * 17
    return jax.shard_map(
        per_device, mesh=mesh, in_specs=in_specs, out_specs=out_specs, check_vma=False
    )
```
